8 devices in a mesh: dp: 1 (over z), tp: 2 (over y), sp: 4 (over x, core).
Axes of the slice: x: 2, y: 2, z: 1, core: 2. Of those that a mesh axis runs over, the one named last changes fastest.
Arguments:
- features: bfloat16 [2, 576, 1024], P('dp', 'sp')
- tokens: int32 [2, 512], P('dp', 'sp')
- lengths: int32 [2], P('dp')
- proj_w: bfloat16 [1024, 2048], replicated
- proj_b: bfloat16 [2048], replicated
- embed: bfloat16 [256000, 2048], P('tp')
- ln_attn: bfloat16 [2, 2048], replicated
- w_query: bfloat16 [2, 2048, 2048], P(None, None, 'tp')
- w_key: bfloat16 [2, 2048, 256], replicated
- w_value: bfloat16 [2, 2048, 256], replicated
- w_out: bfloat16 [2, 2048, 2048], P(None, 'tp')
- ln_mlp: bfloat16 [2, 2048], replicated
- w_gate: bfloat16 [2, 2048, 16384], P(None, None, 'tp')
- w_up: bfloat16 [2, 2048, 16384], P(None, None, 'tp')
- w_down: bfloat16 [2, 16384, 2048], P(None, 'tp')
Outputs:
- output 1: bfloat16 [2, 576, 2048], P('dp', 'sp')
- output 2: bfloat16 [2, 512, 2048], P('dp', 'sp')
- output 3: bfloat16 [2, 2, 2, 576, 256], P(None, None, 'dp', 'sp')
- output 4: bfloat16 [2, 2, 2, 512, 256], P(None, None, 'dp', 'sp')
All inputs are finite; a program needn't handle non-finite values.
Results may differ from the reference program's by a relative error of at most 0.0128077.
Values are sent between devices in bfloat16 or wider.
A program may use at most 3 GiB of HBM per device.

```python
import jax
import jax.numpy as jnp
from jax import lax

BATCH_SIZE = 2
PROMPT_LEN = 512
IMAGE_TOKENS = 576
VISION_WIDTH = 1024
MODEL_WIDTH = 2048
NUM_HEADS = 8
HEAD_DIM = 256
FF_WIDTH = 16384
VOCAB_SIZE = 256000
NUM_LAYERS = 2
DRAW_BLOCKS = 64
SEQ_LEN = IMAGE_TOKENS + PROMPT_LEN
NORM_EPS = 1e-6
ROPE_THETA = 10000.0


def draw_normal(rng_key, arr_shape, std_dev):
    return jax.random.normal(rng_key, arr_shape, jnp.float32) * std_dev


def setup_inputs(seed: int = 0, part: int = 0) -> dict:
    shared_keys = jax.random.split(jax.random.key(seed), 12)
    part_keys = jax.random.split(jax.random.fold_in(jax.random.key(seed + 1), part), 4)
    tokens = jax.random.randint(part_keys[1], (BATCH_SIZE, PROMPT_LEN), 0, VOCAB_SIZE, dtype=jnp.int32)
    drawn_lens = jax.random.randint(part_keys[2], (BATCH_SIZE,), PROMPT_LEN // 4 + 1, PROMPT_LEN + 1, dtype=jnp.int32)
    full_row = jax.random.randint(part_keys[3], (), 0, BATCH_SIZE, dtype=jnp.int32)
    lengths = jnp.where(jnp.arange(BATCH_SIZE) == full_row, PROMPT_LEN, drawn_lens).astype(jnp.int32)
    block_keys = jax.random.split(shared_keys[2], DRAW_BLOCKS)
    embed = lax.map(
        lambda blk_key: draw_normal(blk_key, (VOCAB_SIZE // DRAW_BLOCKS, MODEL_WIDTH), MODEL_WIDTH ** -0.5).astype(jnp.bfloat16),
        block_keys,
    ).reshape(VOCAB_SIZE, MODEL_WIDTH)
    qk_width = NUM_HEADS * HEAD_DIM
    return {
        "features": draw_normal(part_keys[0], (BATCH_SIZE, IMAGE_TOKENS, VISION_WIDTH), 1.0).astype(jnp.bfloat16),
        "tokens": tokens,
        "lengths": lengths,
        "proj_w": draw_normal(shared_keys[0], (VISION_WIDTH, MODEL_WIDTH), VISION_WIDTH ** -0.5).astype(jnp.bfloat16),
        "proj_b": draw_normal(shared_keys[1], (MODEL_WIDTH,), 0.5).astype(jnp.bfloat16),
        "embed": embed,
        "ln_attn": draw_normal(shared_keys[3], (NUM_LAYERS, MODEL_WIDTH), 0.3).astype(jnp.bfloat16),
        "w_query": draw_normal(shared_keys[4], (NUM_LAYERS, MODEL_WIDTH, qk_width), 1.5 * MODEL_WIDTH ** -0.5).astype(jnp.bfloat16),
        "w_key": draw_normal(shared_keys[5], (NUM_LAYERS, MODEL_WIDTH, HEAD_DIM), MODEL_WIDTH ** -0.5).astype(jnp.bfloat16),
        "w_value": draw_normal(shared_keys[6], (NUM_LAYERS, MODEL_WIDTH, HEAD_DIM), MODEL_WIDTH ** -0.5).astype(jnp.bfloat16),
        "w_out": draw_normal(shared_keys[7], (NUM_LAYERS, qk_width, MODEL_WIDTH), (SEQ_LEN / (16.0 * qk_width)) ** 0.5).astype(jnp.bfloat16),
        "ln_mlp": draw_normal(shared_keys[8], (NUM_LAYERS, MODEL_WIDTH), 0.3).astype(jnp.bfloat16),
        "w_gate": draw_normal(shared_keys[9], (NUM_LAYERS, MODEL_WIDTH, FF_WIDTH), MODEL_WIDTH ** -0.5).astype(jnp.bfloat16),
        "w_up": draw_normal(shared_keys[10], (NUM_LAYERS, MODEL_WIDTH, FF_WIDTH), MODEL_WIDTH ** -0.5).astype(jnp.bfloat16),
        "w_down": draw_normal(shared_keys[11], (NUM_LAYERS, FF_WIDTH, MODEL_WIDTH), FF_WIDTH ** -0.5).astype(jnp.bfloat16),
    }


def rms_norm(hidden, norm_gain):
    hid_f32 = hidden.astype(jnp.float32)
    mean_sq = jnp.mean(hid_f32 * hid_f32, axis=-1, keepdims=True)
    return (hid_f32 * lax.rsqrt(mean_sq + NORM_EPS) * (1.0 + norm_gain.astype(jnp.float32))).astype(jnp.bfloat16)


def rotary(vectors, cos_table, sin_table):
    half_dim = vectors.shape[-1] // 2
    first_half = vectors[..., :half_dim]
    second_half = vectors[..., half_dim:]
    return jnp.concatenate([first_half * cos_table - second_half * sin_table, second_half * cos_table + first_half * sin_table], axis=-1)


def reference(features, tokens, lengths, proj_w, proj_b, embed, ln_attn, w_query, w_key, w_value, w_out, ln_mlp, w_gate, w_up, w_down):
    half_dim = HEAD_DIM // 2
    inv_freq = ROPE_THETA ** (-jnp.arange(half_dim, dtype=jnp.float32) * (2.0 / HEAD_DIM))
    angles = jnp.arange(SEQ_LEN, dtype=jnp.float32)[:, None] * inv_freq[None, :]
    cos_table = jnp.cos(angles)
    sin_table = jnp.sin(angles)
    positions = jnp.arange(SEQ_LEN)
    emb_scale = MODEL_WIDTH ** 0.5
    layer_weights = (ln_attn, w_query, w_key, w_value, w_out, ln_mlp, w_gate, w_up, w_down)

    def one_request(request):
        feat_req, tok_req, len_req = request
        img_rows = (jnp.dot(feat_req, proj_w, preferred_element_type=jnp.float32) + proj_b.astype(jnp.float32)).astype(jnp.bfloat16)
        txt_rows = (jnp.take(embed, tok_req, axis=0).astype(jnp.float32) * emb_scale).astype(jnp.bfloat16)
        hidden_start = jnp.concatenate([img_rows, txt_rows], axis=0)
        key_valid = positions < IMAGE_TOKENS + len_req

        def layer_step(hidden, weights):
            gain_attn, wq_layer, wk_layer, wv_layer, wo_layer, gain_mlp, wg_layer, wu_layer, wd_layer = weights
            normed = rms_norm(hidden, gain_attn)
            queries = jnp.dot(normed, wq_layer, preferred_element_type=jnp.float32).reshape(SEQ_LEN, NUM_HEADS, HEAD_DIM)
            queries = rotary(queries, cos_table[:, None, :], sin_table[:, None, :]).astype(jnp.bfloat16)
            key_rows = rotary(jnp.dot(normed, wk_layer, preferred_element_type=jnp.float32), cos_table, sin_table).astype(jnp.bfloat16)
            value_rows = jnp.dot(normed, wv_layer, preferred_element_type=jnp.float32).astype(jnp.bfloat16)

            def attend_head(head_query):
                scores = jnp.dot(head_query, key_rows.T, preferred_element_type=jnp.float32) * HEAD_DIM ** -0.5
                scores = jnp.where(key_valid[None, :], scores, -1e30)
                attn_probs = jax.nn.softmax(scores, axis=-1).astype(jnp.bfloat16)
                return jnp.dot(attn_probs, value_rows, preferred_element_type=jnp.float32).astype(jnp.bfloat16)

            attn_heads = lax.map(attend_head, jnp.transpose(queries, (1, 0, 2)))
            attn_heads = jnp.transpose(attn_heads, (1, 0, 2)).reshape(SEQ_LEN, NUM_HEADS * HEAD_DIM)
            attn_out = jnp.dot(attn_heads, wo_layer, preferred_element_type=jnp.float32).astype(jnp.bfloat16)
            hidden = (hidden.astype(jnp.float32) + attn_out.astype(jnp.float32)).astype(jnp.bfloat16)
            normed = rms_norm(hidden, gain_mlp)
            gate_pre = jnp.dot(normed, wg_layer, preferred_element_type=jnp.float32)
            up_proj = jnp.dot(normed, wu_layer, preferred_element_type=jnp.float32)
            mlp_mix = (jax.nn.gelu(gate_pre, approximate=True) * up_proj).astype(jnp.bfloat16)
            down_out = jnp.dot(mlp_mix, wd_layer, preferred_element_type=jnp.float32).astype(jnp.bfloat16)
            hidden = (hidden.astype(jnp.float32) + down_out.astype(jnp.float32)).astype(jnp.bfloat16)
            return hidden, jnp.stack([key_rows, value_rows])

        return lax.scan(layer_step, hidden_start, layer_weights)

    hidden_all, cache_all = lax.map(one_request, (features, tokens, lengths))
    cache_all = jnp.transpose(cache_all, (1, 2, 0, 3, 4))
    return (hidden_all[:, :IMAGE_TOKENS], hidden_all[:, IMAGE_TOKENS:], cache_all[:, :, :, :IMAGE_TOKENS], cache_all[:, :, :, IMAGE_TOKENS:])
```

```python
import math
import jax
import jax.numpy as jnp
from jax import lax
from jax.sharding import PartitionSpec as P

NORM_EPS = 1e-6
ROPE_THETA = 10000.0
NUM_LAYERS = 2
SWAP = [(0, 1), (1, 0)]


def rms_norm(hidden, norm_gain):
    hid_f32 = hidden.astype(jnp.float32)
    mean_sq = jnp.mean(hid_f32 * hid_f32, axis=-1, keepdims=True)
    return (hid_f32 * lax.rsqrt(mean_sq + NORM_EPS) * (1.0 + norm_gain.astype(jnp.float32))).astype(jnp.bfloat16)


def rotary(vectors, cos_table, sin_table):
    half_dim = vectors.shape[-1] // 2
    first_half = vectors[..., :half_dim]
    second_half = vectors[..., half_dim:]
    return jnp.concatenate([first_half * cos_table - second_half * sin_table, second_half * cos_table + first_half * sin_table], axis=-1)


def rope_tables(positions, head_dim):
    half_dim = head_dim // 2
    inv_freq = ROPE_THETA ** (-jnp.arange(half_dim, dtype=jnp.float32) * (2.0 / head_dim))
    angles = positions.astype(jnp.float32)[:, None] * inv_freq[None, :]
    return jnp.cos(angles), jnp.sin(angles)


def dot32(a, b):
    return jnp.dot(a, b, preferred_element_type=jnp.float32)


def exchange_add(hidden, part):
    other = lax.ppermute(part, "tp", SWAP)
    total = (part.astype(jnp.float32) + other.astype(jnp.float32)).astype(jnp.bfloat16)
    return (hidden.astype(jnp.float32) + total.astype(jnp.float32)).astype(jnp.bfloat16)


def solution(mesh):
    sp_size = mesh.shape["sp"]
    in_specs = (P("dp", "sp", None), P("dp", "sp"), P("dp"), P(), P(), P("tp", None), P(), P(None, None, "tp"), P(), P(), P(None, "tp", None), P(), P(None, None, "tp"), P(None, None, "tp"), P(None, "tp", None))
    out_specs = (P("dp", "sp", None), P("dp", "sp", None), P(None, None, "dp", "sp", None), P(None, None, "dp", "sp", None))

    def device_fn(features, tokens, lengths, proj_w, proj_b, embed, ln_attn, w_query, w_key, w_value, w_out, ln_mlp, w_gate, w_up, w_down):
        num_req, img_loc, _ = features.shape
        txt_loc = tokens.shape[1]
        seq_loc = img_loc + txt_loc
        model_width = proj_w.shape[1]
        head_dim = w_key.shape[2]
        heads_loc = w_query.shape[2] // head_dim
        rows_loc = embed.shape[0]
        shard_idx = lax.axis_index("sp")
        tp_idx = lax.axis_index("tp")

        positions = jnp.concatenate([shard_idx * img_loc + jnp.arange(img_loc), img_loc * sp_size + shard_idx * txt_loc + jnp.arange(txt_loc)])
        cos_table, sin_table = rope_tables(positions, head_dim)
        slot_idx = jnp.arange(seq_loc)[None, :]
        text_index = jnp.arange(sp_size)[:, None] * txt_loc + slot_idx - img_loc

        hidden, key_valid = [], []
        for req in range(num_req):
            local_ids = tokens[req] - tp_idx * rows_loc
            owned_row = (local_ids >= 0) & (local_ids < rows_loc)
            picked = jnp.take(embed, jnp.clip(local_ids, 0, rows_loc - 1), axis=0)
            picked = jnp.where(owned_row[:, None], picked, jnp.zeros((), jnp.bfloat16))
            both = picked.astype(jnp.float32) + lax.ppermute(picked, "tp", SWAP).astype(jnp.float32)
            txt_rows = (both * math.sqrt(model_width)).astype(jnp.bfloat16)
            img_rows = (dot32(features[req], proj_w) + proj_b.astype(jnp.float32)).astype(jnp.bfloat16)
            hidden.append(jnp.concatenate([img_rows, txt_rows], axis=0))
            key_valid.append(((slot_idx < img_loc) | (text_index < lengths[req])).reshape(sp_size * seq_loc))

        cache_parts = []
        for layer_idx in range(NUM_LAYERS):
            kv_rows = []
            for req in range(num_req):
                normed = rms_norm(hidden[req], ln_attn[layer_idx])
                key_rows = rotary(dot32(normed, w_key[layer_idx]), cos_table, sin_table).astype(jnp.bfloat16)
                value_rows = dot32(normed, w_value[layer_idx]).astype(jnp.bfloat16)
                kv_rows.append(jnp.stack([key_rows, value_rows]))
                kv_all = lax.all_gather(jnp.concatenate([key_rows, value_rows], axis=-1), "sp", axis=0, tiled=True)
                queries = dot32(normed, w_query[layer_idx])
                heads = []
                for head in range(heads_loc):
                    query = rotary(queries[:, head * head_dim:(head + 1) * head_dim], cos_table, sin_table).astype(jnp.bfloat16)
                    scores = lax.dot_general(query, kv_all[:, :head_dim], (((1,), (1,)), ((), ())), preferred_element_type=jnp.float32) * head_dim ** -0.5
                    scores = jnp.where(key_valid[req][None, :], scores, -1e30)
                    probs = jax.nn.softmax(scores, axis=-1).astype(jnp.bfloat16)
                    heads.append(dot32(probs, kv_all[:, head_dim:]).astype(jnp.bfloat16))
                attn_part = dot32(jnp.concatenate(heads, axis=-1), w_out[layer_idx]).astype(jnp.bfloat16)
                hidden[req] = exchange_add(hidden[req], attn_part)
            for req in range(num_req):
                normed = rms_norm(hidden[req], ln_mlp[layer_idx])
                gate_pre = dot32(normed, w_gate[layer_idx])
                up_proj = dot32(normed, w_up[layer_idx])
                mlp_mix = (jax.nn.gelu(gate_pre, approximate=True) * up_proj).astype(jnp.bfloat16)
                hidden[req] = exchange_add(hidden[req], dot32(mlp_mix, w_down[layer_idx]).astype(jnp.bfloat16))
            cache_parts.append(jnp.stack(kv_rows, axis=1))
        cache_loc = jnp.stack(cache_parts)
        hidden = jnp.stack(hidden)
        return hidden[:, :img_loc], hidden[:, img_loc:], cache_loc[:, :, :, :img_loc], cache_loc[:, :, :, img_loc:]

    return jax.shard_map(device_fn, mesh=mesh, in_specs=in_specs, out_specs=out_specs, check_vma=False)
```

```python
import functools
import math
import jax
import jax.numpy as jnp
from jax import lax
from jax.experimental import pallas as pl
from jax.experimental.pallas import tpu as pltpu
from jax.sharding import PartitionSpec as P

NORM_EPS = 1e-6
ROPE_THETA = 10000.0
NUM_LAYERS = 2
SWAP = [(0, 1), (1, 0)]
ROW_BLOCK = 16
MASKED = -1e30


def rope_tables(positions, head_dim):
    half_dim = head_dim // 2
    inv_freq = ROPE_THETA ** (-jnp.arange(half_dim, dtype=jnp.float32) * (2.0 / head_dim))
    angles = positions.astype(jnp.float32)[:, None] * inv_freq[None, :]
    return jnp.cos(angles), jnp.sin(angles)


def dot32(a, b):
    return jnp.dot(a, b, preferred_element_type=jnp.float32)


def f32(a):
    return a.astype(jnp.float32)


def bf16(a):
    return a.astype(jnp.bfloat16)


def gelu_tanh(x):
    return x * (0.5 * (1.0 + jnp.tanh(math.sqrt(2.0 / math.pi) * (x + 0.044715 * (x * x * x)))))


def add_parts(hidden, own, other):
    return bf16(f32(hidden) + f32(bf16(f32(own) + f32(other))))


def ds(start, size):
    return pl.ds(pl.multiple_of(start, size), size)


def norm_rows(parts, hid, gain, hid_out, x):
    scale = 1.0 + f32(gain[...])

    @pl.loop(0, hid.shape[0] // ROW_BLOCK)
    def _(blk):
        rows = ds(blk * ROW_BLOCK, ROW_BLOCK)
        h = hid[rows, :]
        if parts:
            h = add_parts(h, parts[0][rows, :], parts[1][rows, :])
            hid_out[rows, :] = h
        h = f32(h)
        x[rows, :] = bf16(h * lax.rsqrt(jnp.mean(h * h, axis=-1, keepdims=True) + NORM_EPS) * scale)


def attention_kernel(layer, has_parts, img_loc, *refs):
    parts, refs = (refs[:2], refs[2:]) if has_parts else ((), refs)
    hid, gain, cos, sin, length, wq, wk, wv, wo, *refs = refs
    hid_out, refs = (refs[0], refs[1:]) if has_parts else (None, refs)
    kv_out, part, x, kvs, q, o, wq_buf, wk_buf, wv_buf, wo_buf, wsem, send_sem, recv_sem = refs
    rows = hid.shape[0]
    head_dim = wk.shape[2]
    half = head_dim // 2
    heads = wq.shape[2] // head_dim
    txt_loc = rows - img_loc
    me = lax.axis_index("sp")
    core, chip = lax.bitwise_xor(me, 1), lax.bitwise_xor(me, 2)

    loads = [pltpu.make_async_copy(src.at[layer], dst, wsem.at[i]) for i, (src, dst) in enumerate(((wk, wk_buf), (wv, wv_buf), (wq, wq_buf), (wo, wo_buf)))]
    for load in loads:
        load.start()
    barrier = pltpu.get_barrier_semaphore()
    for peer in (core, chip):
        pl.semaphore_signal(barrier, inc=1, device_id={"sp": peer}, device_id_type=pl.DeviceIdType.MESH)

    norm_rows(parts, hid, gain, hid_out, x)

    def rope(v):
        first, second = v[:, :half], v[:, half:]
        return first * cos[...] - second * sin[...], second * cos[...] + first * sin[...]

    loads[0].wait()
    first, second = rope(dot32(x[...], wk_buf[...]))
    kvs[:rows, :half] = bf16(first)
    kvs[:rows, half:head_dim] = bf16(second)
    loads[1].wait()
    kvs[:rows, head_dim:] = bf16(dot32(x[...], wv_buf[...]))
    pl.semaphore_wait(barrier, 2)

    def send(i, src, dst, peer):
        return pltpu.make_async_remote_copy(src_ref=kvs.at[pl.ds(src * rows, rows)], dst_ref=kvs.at[pl.ds(dst * rows, rows)], send_sem=send_sem.at[i], recv_sem=recv_sem.at[i], device_id={"sp": peer}, device_id_type=pl.DeviceIdType.MESH)

    to_chip, to_core, relay = send(0, 0, 2, chip), send(1, 0, 1, core), send(2, 2, 3, core)
    to_chip.start()
    to_core.start()
    kv_out[...] = kvs[:rows, :]

    loads[2].wait()
    for head in range(heads):
        lanes = slice(head * head_dim, (head + 1) * head_dim)
        first, second = rope(dot32(x[...], wq_buf[:, lanes]))
        q[:, head * head_dim:head * head_dim + half] = bf16(bf16(first) * head_dim ** -0.5)
        q[:, head * head_dim + half:(head + 1) * head_dim] = bf16(bf16(second) * head_dim ** -0.5)

    to_chip.wait_recv()
    relay.start()
    col = lax.broadcasted_iota(jnp.int32, (1, 4 * rows), 1)
    slot = (col >= rows).astype(jnp.int32) + (col >= 2 * rows).astype(jnp.int32) + (col >= 3 * rows).astype(jnp.int32)
    idx = col - slot * rows
    owner = jnp.where(slot == 0, me, jnp.where(slot == 1, core, jnp.where(slot == 2, chip, lax.bitwise_xor(me, 3))))
    valid = (idx < img_loc) | (owner * txt_loc + idx - img_loc < length[0])
    to_core.wait_recv()
    relay.wait_recv()

    for head in range(heads):
        lanes = slice(head * head_dim, (head + 1) * head_dim)
        s = lax.dot_general(q[:, lanes], kvs[:, :head_dim], (((1,), (1,)), ((), ())), preferred_element_type=jnp.float32)
        s = jnp.where(valid, s, MASKED)
        e = jnp.exp(s - jnp.max(s, axis=-1, keepdims=True))
        p = bf16(e * (1.0 / jnp.sum(e, axis=-1, keepdims=True)))
        o[:, lanes] = bf16(dot32(p, kvs[:, head_dim:]))

    loads[3].wait()
    tile = 2 * head_dim
    for n in range(wo.shape[2] // tile):
        part[:, n * tile:(n + 1) * tile] = bf16(dot32(o[...], wo_buf[:, n * tile:(n + 1) * tile]))
    for copy in (to_chip, to_core, relay):
        copy.wait_send()


def attention(parts, hid, gain, cos, sin, length, wq, wk, wv, wo, layer, img_loc):
    rows, width = hid.shape
    qw, kw = wq.shape[2], wk.shape[2]
    vm = pl.BlockSpec(memory_space=pltpu.VMEM)
    anywhere = pl.BlockSpec(memory_space=pl.ANY)
    hid_shape = jax.ShapeDtypeStruct((rows, width), jnp.bfloat16)
    kv_shape = jax.ShapeDtypeStruct((rows, 2 * kw), jnp.bfloat16)
    outs = ((hid_shape,) if parts else ()) + (kv_shape, hid_shape)
    res = pl.pallas_call(
        functools.partial(attention_kernel, layer, bool(parts), img_loc),
        out_shape=outs,
        in_specs=[vm] * (len(parts) + 4) + [pl.BlockSpec(memory_space=pltpu.SMEM)] + [anywhere] * 4,
        out_specs=(vm,) * len(outs),
        scratch_shapes=[
            pltpu.VMEM((rows, width), jnp.bfloat16),
            pltpu.VMEM((4 * rows, 2 * kw), jnp.bfloat16),
            pltpu.VMEM((rows, qw), jnp.bfloat16),
            pltpu.VMEM((rows, qw), jnp.bfloat16),
            pltpu.VMEM((width, qw), jnp.bfloat16),
            pltpu.VMEM((width, kw), jnp.bfloat16),
            pltpu.VMEM((width, kw), jnp.bfloat16),
            pltpu.VMEM((qw, width), jnp.bfloat16),
            pltpu.SemaphoreType.DMA((4,)),
            pltpu.SemaphoreType.DMA((3,)),
            pltpu.SemaphoreType.DMA((3,)),
        ],
        compiler_params=pltpu.CompilerParams(collective_id=layer, has_side_effects=True, vmem_limit_bytes=40 << 20),
        cost_estimate=pl.CostEstimate(flops=12_000_000_000, bytes_accessed=2 * (2 * width * qw + 2 * width * kw), transcendentals=rows * rows * 16),
        name=f"attention{layer}",
    )(*parts, hid, gain, cos, sin, length, wq, wk, wv, wo)
    return res if parts else (hid, *res)


def mlp_kernel(layer, tf, tn, own, other, hid, gain, wg, wu, wd, hid_out, part, x, act, gbuf, ubuf, dbuf, gsem, usem, dsem):
    ff, width = wd.shape[1:]
    nf, nn = ff // tf, width // tn
    nb, nd = gbuf.shape[0], dbuf.shape[0]

    def load(src, buf, sem, tile, i, slot):
        return pltpu.make_async_copy(src.at[layer, :, ds(i * tile, tile)], buf.at[slot], sem.at[slot])

    gload = functools.partial(load, wg, gbuf, gsem, tf)
    uload = functools.partial(load, wu, ubuf, usem, tf)
    dload = functools.partial(load, wd, dbuf, dsem, tn)
    for i in range(nb):
        gload(i, i).start()
        uload(i, i).start()
    norm_rows((own, other), hid, gain, hid_out, x)

    @pl.loop(0, nf)
    def _(i):
        slot = lax.rem(i, nb)
        gload(i, slot).wait()
        gate = dot32(x[...], gbuf[slot])
        uload(i, slot).wait()
        act[:, ds(i * tf, tf)] = bf16(gelu_tanh(gate) * dot32(x[...], ubuf[slot]))

        @pl.when(i + nb < nf)
        def _():
            gload(i + nb, slot).start()
            uload(i + nb, slot).start()

        @pl.when((i + nb >= nf) & (i + nb < nf + nd))
        def _():
            dload(i + nb - nf, i + nb - nf).start()

    @pl.loop(0, nn)
    def _(i):
        slot = lax.rem(i, nd)
        dload(i, slot).wait()
        part[:, ds(i * tn, tn)] = bf16(dot32(act[...], dbuf[slot]))

        @pl.when(i + nd < nn)
        def _():
            dload(i + nd, slot).start()


def mlp(own, other, hid, gain, wg, wu, wd, layer, tf=1024, tn=512, nb=2, nd=2):
    rows, width = hid.shape
    ff = wg.shape[2]
    vm = pl.BlockSpec(memory_space=pltpu.VMEM)
    anywhere = pl.BlockSpec(memory_space=pl.ANY)
    hid_shape = jax.ShapeDtypeStruct((rows, width), jnp.bfloat16)
    return pl.pallas_call(
        functools.partial(mlp_kernel, layer, tf, tn),
        out_shape=(hid_shape, hid_shape),
        in_specs=[vm] * 4 + [anywhere] * 3,
        out_specs=(vm, vm),
        scratch_shapes=[
            pltpu.VMEM((rows, width), jnp.bfloat16),
            pltpu.VMEM((rows, ff), jnp.bfloat16),
            pltpu.VMEM((nb, width, tf), jnp.bfloat16),
            pltpu.VMEM((nb, width, tf), jnp.bfloat16),
            pltpu.VMEM((nd, ff, tn), jnp.bfloat16),
            pltpu.SemaphoreType.DMA((nb,)),
            pltpu.SemaphoreType.DMA((nb,)),
            pltpu.SemaphoreType.DMA((nd,)),
        ],
        compiler_params=pltpu.CompilerParams(vmem_limit_bytes=54 << 20),
        cost_estimate=pl.CostEstimate(flops=6 * rows * width * ff, bytes_accessed=6 * width * ff, transcendentals=rows * ff),
        name=f"mlp{layer}",
    )(own, other, hid, gain, wg, wu, wd)


def solution(mesh):
    sp_size = mesh.shape["sp"]
    in_specs = (P("dp", "sp", None), P("dp", "sp"), P("dp"), P(), P(), P("tp", None), P(), P(None, None, "tp"), P(), P(), P(None, "tp", None), P(), P(None, None, "tp"), P(None, None, "tp"), P(None, "tp", None))
    out_specs = (P("dp", "sp", None), P("dp", "sp", None), P(None, None, "dp", "sp", None), P(None, None, "dp", "sp", None))

    def device_fn(features, tokens, lengths, proj_w, proj_b, embed, ln_attn, w_query, w_key, w_value, w_out, ln_mlp, w_gate, w_up, w_down):
        num_req, img_loc, _ = features.shape
        txt_loc = tokens.shape[1]
        model_width = proj_w.shape[1]
        head_dim = w_key.shape[2]
        rows_loc = embed.shape[0]
        shard_idx = lax.axis_index("sp")
        tp_idx = lax.axis_index("tp")
        reqs = range(num_req)

        positions = jnp.concatenate([shard_idx * img_loc + jnp.arange(img_loc), img_loc * sp_size + shard_idx * txt_loc + jnp.arange(txt_loc)])
        cos_table, sin_table = rope_tables(positions, head_dim)

        hidden = []
        for req in reqs:
            local_ids = tokens[req] - tp_idx * rows_loc
            owned_row = (local_ids >= 0) & (local_ids < rows_loc)
            picked = jnp.take(embed, jnp.clip(local_ids, 0, rows_loc - 1), axis=0)
            picked = jnp.where(owned_row[:, None], picked, jnp.zeros((), jnp.bfloat16))
            txt_rows = bf16((f32(picked) + f32(lax.ppermute(picked, "tp", SWAP))) * math.sqrt(model_width))
            img_rows = bf16(dot32(features[req], proj_w) + f32(proj_b))
            hidden.append(jnp.concatenate([img_rows, txt_rows], axis=0))

        parts = [()] * num_req
        cache_parts = []
        for layer in range(NUM_LAYERS):
            kvs = [None] * num_req
            for req in reqs:
                hidden[req], kvs[req], part = attention(parts[req], hidden[req], ln_attn[layer:layer + 1], cos_table, sin_table, lengths[req:req + 1], w_query, w_key, w_value, w_out, layer, img_loc)
                parts[req] = (part, lax.ppermute(part, "tp", SWAP))
            for req in reqs:
                hidden[req], part = mlp(*parts[req], hidden[req], ln_mlp[layer:layer + 1], w_gate, w_up, w_down, layer)
                parts[req] = (part, lax.ppermute(part, "tp", SWAP))
            cache_parts.append(jnp.stack(kvs))
        cache = jnp.stack(cache_parts)
        cache = jnp.stack([cache[..., :head_dim], cache[..., head_dim:]], axis=1)
        hidden = jnp.stack([add_parts(hidden[req], *parts[req]) for req in reqs])
        return hidden[:, :img_loc], hidden[:, img_loc:], cache[:, :, :, :img_loc], cache[:, :, :, img_loc:]

    return jax.shard_map(device_fn, mesh=mesh, in_specs=in_specs, out_specs=out_specs, check_vma=False)
```

```python
import functools
import math
import numpy as np
import jax
import jax.numpy as jnp
from jax import lax
from jax.experimental import pallas as pl
from jax.experimental.pallas import tpu as pltpu
from jax.sharding import PartitionSpec as P

NORM_EPS = 1e-6
ROPE_THETA = 10000.0
NUM_LAYERS = 2
NUM_REQ = 2
BLOCK = 16
GROUP = 8
MASKED = -1e30
MESH_ID = pl.DeviceIdType.MESH
VMEM_SPEC = pl.BlockSpec(memory_space=pltpu.VMEM)
SMEM_SPEC = pl.BlockSpec(memory_space=pltpu.SMEM)
ANY_SPEC = pl.BlockSpec(memory_space=pl.ANY)
DMA = pltpu.SemaphoreType.DMA


def vmem(*shape):
    return pltpu.VMEM(shape, jnp.bfloat16)


def out(*shape):
    return jax.ShapeDtypeStruct(shape, jnp.bfloat16)


def dot32(a, b):
    return jnp.dot(a, b, preferred_element_type=jnp.float32)


def f32(a):
    return a.astype(jnp.float32)


def bf16(a):
    return a.astype(jnp.bfloat16)


def gelu_tanh(x):
    return x * (0.5 * (1.0 + jnp.tanh(math.sqrt(2.0 / math.pi) * (x + 0.044715 * (x * x * x)))))


def add_parts(hidden, own, other):
    return bf16(f32(hidden) + f32(bf16(f32(own) + f32(other))))


def normed(h, scale):
    h = f32(h)
    return bf16(h * lax.rsqrt(jnp.mean(h * h, axis=-1, keepdims=True) + NORM_EPS) * scale)


def ds(start, size, multiple=None):
    return pl.ds(pl.multiple_of(start, multiple or size), size)


def each_block(rows, body):
    @pl.loop(0, rows // BLOCK)
    def _(blk):
        body(lambda base: ds(base + blk * BLOCK, BLOCK))


def greet(peers):
    barrier = pltpu.get_barrier_semaphore()
    for peer in peers:
        pl.semaphore_signal(barrier, inc=1, device_id=peer, device_id_type=MESH_ID)
    pl.semaphore_wait(barrier, len(peers))


def remote(src, dst, send_sem, recv_sem, peer):
    return pltpu.make_async_remote_copy(src_ref=src, dst_ref=dst, send_sem=send_sem, recv_sem=recv_sem, device_id=peer, device_id_type=MESH_ID)


def start_kernel(ids, id_col, features, bias, proj, embed, img, picked, groups, proj_buf, gsem, psem):
    rows_loc = embed.shape[0]
    num = ids.shape[0]
    lo = lax.axis_index("tp") * rows_loc
    load = pltpu.make_async_copy(proj, proj_buf, psem)

    def fetch(i, row):
        return pltpu.make_async_copy(embed.at[ds(row, GROUP)], groups.at[i], gsem)

    @pl.loop(0, num)
    def _(i):
        row = jnp.clip(ids[i] - lo, 0, rows_loc - 1)
        fetch(i, row - lax.rem(row, GROUP)).start()

    load.start()
    load.wait()
    tile = 512
    for n in range(proj.shape[1] // tile):
        cols = slice(n * tile, (n + 1) * tile)
        img[:, cols] = bf16(dot32(features[...], proj_buf[:, cols]) + f32(bias[:, cols]))

    pltpu.make_async_copy(groups, groups, gsem).wait()

    part = 64
    sub = lax.broadcasted_iota(jnp.int32, (part, part * GROUP), 0)
    col = lax.broadcasted_iota(jnp.int32, (part, part * GROUP), 1)
    for p in range(num // part):
        rel = id_col[p * part:(p + 1) * part, :] - lo
        want = jnp.where((rel >= 0) & (rel < rows_loc), rel & (GROUP - 1), -GROUP * part * 2)
        pick = jnp.where(col == sub * GROUP + want, 1.0, 0.0).astype(jnp.bfloat16)
        rows = groups[p * part:(p + 1) * part].reshape(part * GROUP, groups.shape[2])
        picked[p * part:(p + 1) * part, :] = bf16(dot32(pick, rows))


def start(tokens, features, proj_w, proj_b, embed):
    num = tokens.size
    vis, width = proj_w.shape
    feats = features.reshape(-1, vis)
    return pl.pallas_call(
        start_kernel,
        out_shape=(out(feats.shape[0], width), out(num, width)),
        in_specs=[SMEM_SPEC, VMEM_SPEC, VMEM_SPEC, VMEM_SPEC, ANY_SPEC, ANY_SPEC],
        out_specs=(VMEM_SPEC, VMEM_SPEC),
        scratch_shapes=[vmem(num, GROUP, width), vmem(vis, width), DMA, DMA],
        compiler_params=pltpu.CompilerParams(vmem_limit_bytes=32 << 20),
        name="start",
    )(tokens.reshape(num), tokens.reshape(num, 1), feats, proj_b.reshape(1, width), proj_w, embed)


def attention_kernel(layer, img_loc, *refs):
    first = layer == 0
    refs, refs_in = (refs[2:], refs[:2]) if first else (refs[4:], refs[:4])
    gain, cos, sin, lengths, wq, wk, wv, wo, hid, kv, part, recv, x, arrive, kvs, q, o, wq_buf, wk_buf, wv_buf, wo_buf, wsem, tp_send, tp_recv, sp_send, sp_recv = refs
    rows = hid.shape[0] // NUM_REQ
    txt_loc = rows - img_loc
    head_dim = wk.shape[2]
    half = head_dim // 2
    heads = wq.shape[2] // head_dim
    width = hid.shape[1]
    me = lax.axis_index("sp")
    twin = {"tp": 1 - lax.axis_index("tp")}
    near, far, cross = [lax.bitwise_xor(me, k) for k in (1, 2, 3)]

    loads = [pltpu.make_async_copy(src.at[layer], dst, wsem.at[i]) for i, (src, dst) in enumerate(((wk, wk_buf), (wv, wv_buf), (wq, wq_buf), (wo, wo_buf)))]
    loads[0].start()
    loads[1].start()
    greet(({"sp": near}, {"sp": far}, twin))
    if first:
        img, picked = refs_in
        span = [pl.ds(req * txt_loc, txt_loc) for req in range(NUM_REQ)]
        arrivals = [remote(picked.at[span[req]], arrive.at[span[req]], tp_send.at[req], tp_recv.at[req], twin) for req in range(NUM_REQ)]
    else:
        hid_in, mlp_part, mlp_recv, mlp_tile = refs_in
        done = mlp_tile.shape[1]
        arrivals = [None, remote(mlp_part.at[pl.ds(rows, rows), pl.ds(done, width - done)], arrive.at[:, pl.ds(done, width - done)], tp_send.at[1], tp_recv.at[1], twin)]
    for arrival in arrivals:
        if arrival is not None:
            arrival.start()
    scale = 1.0 + f32(gain[...])

    def keep(at, local, h):
        hid[at, :] = h
        x[local, :] = normed(h, scale)

    def embedded(req):
        def image(at):
            keep(at(req * rows), at(0), img[at(req * img_loc), :])

        def prompt(at):
            src = at(req * txt_loc)
            keep(at(req * rows + img_loc), at(img_loc), bf16((f32(picked[src, :]) + f32(arrive[src, :])) * math.sqrt(width)))

        each_block(img_loc, image)
        arrivals[req].wait_recv()
        each_block(txt_loc, prompt)

    def continued(req):
        other = mlp_recv if req == 0 else arrive
        if req == 1:
            arrive[:, :done] = mlp_tile[...]
            arrivals[1].wait_recv()

        def row_block(at):
            src = at(req * rows)
            keep(src, at(0), add_parts(hid_in[src, :], mlp_part[src, :], other[at(0), :]))

        each_block(rows, row_block)

    def rope(v):
        a, b = v[:, :half], v[:, half:]
        return a * cos[...] - b * sin[...], b * cos[...] + a * sin[...]

    def before(req):
        (embedded if first else continued)(req)
        slots = [pl.ds((req * 4 + k) * rows, rows) for k in range(4)]
        if req == 0:
            loads[0].wait()
            loads[2].start()
            loads[3].start()
        a, b = rope(dot32(x[...], wk_buf[...]))
        kvs[slots[0], :half] = bf16(a)
        kvs[slots[0], half:head_dim] = bf16(b)
        if req == 0:
            loads[1].wait()
        kvs[slots[0], head_dim:] = bf16(dot32(x[...], wv_buf[...]))
        sends = [remote(kvs.at[slots[src]], kvs.at[slots[dst]], sp_send.at[req * 3 + i], sp_recv.at[req * 3 + i], {"sp": peer}) for i, (src, dst, peer) in enumerate(((0, 2, far), (0, 1, near), (2, 3, near)))]
        sends[0].start()
        sends[1].start()
        kv[pl.ds(req * rows, rows), :] = kvs[slots[0], :]
        if req == 0:
            loads[2].wait()
        for head in range(heads):
            base = head * head_dim
            a, b = rope(dot32(x[...], wq_buf[:, base:base + head_dim]))
            q[:, base:base + half] = bf16(bf16(a) * head_dim ** -0.5)
            q[:, base + half:base + head_dim] = bf16(bf16(b) * head_dim ** -0.5)
        return sends

    col = lax.broadcasted_iota(jnp.int32, (1, 4 * rows), 1)
    slot = (col >= rows).astype(jnp.int32) + (col >= 2 * rows).astype(jnp.int32) + (col >= 3 * rows).astype(jnp.int32)
    owner = jnp.where(slot == 0, me, jnp.where(slot == 1, near, jnp.where(slot == 2, far, cross)))
    idx = col - slot * rows
    text_pos = jnp.where(idx < img_loc, -1, owner * txt_loc + idx - img_loc)

    def after(req, sends):
        sends[0].wait_recv()
        sends[2].start()
        sends[1].wait_recv()
        sends[2].wait_recv()
        valid = text_pos < lengths[req]
        every = pl.ds(req * 4 * rows, 4 * rows)
        for head in range(heads):
            lanes = slice(head * head_dim, (head + 1) * head_dim)
            s = lax.dot_general(q[:, lanes], kvs[every, :head_dim], (((1,), (1,)), ((), ())), preferred_element_type=jnp.float32)
            s = jnp.where(valid, s, MASKED)
            e = jnp.exp(s - jnp.max(s, axis=-1, keepdims=True))
            p = bf16(e * (1.0 / jnp.sum(e, axis=-1, keepdims=True)))
            o[:, lanes] = bf16(dot32(p, kvs[every, head_dim:]))
        if req == 0:
            loads[3].wait()
        tile = 2 * head_dim
        for n in range(width // tile):
            cols = slice(n * tile, (n + 1) * tile)
            part[pl.ds(req * rows, rows), cols] = bf16(dot32(o[...], wo_buf[:, cols]))

    swap = remote(part.at[pl.ds(0, rows)], recv, tp_send.at[2], tp_recv.at[2], twin)
    sends = before(0)
    after(0, sends)
    swap.start()
    more = before(1)
    after(1, more)
    swap.wait_recv()
    for copy in (*sends, *more, *[a for a in arrivals if a is not None], swap):
        copy.wait_send()


def attention(sources, gain, cos, sin, lengths, wq, wk, wv, wo, layer, img_loc):
    rows = cos.shape[0]
    width, qw = wq.shape[1:]
    kw = wk.shape[2]
    arrive_rows = sources[1].shape[0] if layer == 0 else rows
    return pl.pallas_call(
        functools.partial(attention_kernel, layer, img_loc),
        out_shape=(out(NUM_REQ * rows, width), out(NUM_REQ * rows, 2 * kw), out(NUM_REQ * rows, width), out(rows, width)),
        in_specs=[VMEM_SPEC] * (len(sources) + 3) + [SMEM_SPEC] + [ANY_SPEC] * 4,
        out_specs=(VMEM_SPEC,) * 4,
        scratch_shapes=[
            vmem(rows, width), vmem(arrive_rows, width), vmem(NUM_REQ * 4 * rows, 2 * kw), vmem(rows, qw), vmem(rows, qw),
            vmem(width, qw), vmem(width, kw), vmem(width, kw), vmem(qw, width),
            DMA((4,)), DMA((3,)), DMA((3,)), DMA((6,)), DMA((6,)),
        ],
        compiler_params=pltpu.CompilerParams(collective_id=layer, has_side_effects=True, vmem_limit_bytes=48 << 20),
        name=f"attention{layer}",
    )(*sources, gain, cos, sin, lengths, wq, wk, wv, wo)


def mlp_kernel(layer, img_loc, tf, tn, hid_in, own, recv0, gain, wg, wu, wd, *refs):
    last = layer == NUM_LAYERS - 1
    if last:
        image, prompt, hid, part, recv, tiles, *refs = refs
    else:
        hid, part, recv, tiles, *refs = refs
    other, x, act, gbuf, ubuf, dbuf, gsem, usem, dsem, tp_send, tp_recv = refs
    rows = recv0.shape[0]
    ff, width = wd.shape[1:]
    nf, nn = ff // tf, width // tn
    nb, nd = gbuf.shape[0], dbuf.shape[0]
    streamed = nn if last else 1
    twin = {"tp": 1 - lax.axis_index("tp")}

    def load(src, buf, sem, tile, i, slot):
        return pltpu.make_async_copy(src.at[layer, :, ds(i * tile, tile)], buf.at[slot], sem.at[slot])

    gload = functools.partial(load, wg, gbuf, gsem, tf)
    uload = functools.partial(load, wu, ubuf, usem, tf)
    dload = functools.partial(load, wd, dbuf, dsem, tn)
    for i in range(nb):
        gload(i, i).start()
        uload(i, i).start()
    greet((twin,))
    upper = pl.ds(rows, rows)
    incoming = remote(own.at[upper], other.at[upper], tp_send.at[0], tp_recv.at[0], twin)
    incoming.start()
    swap = remote(part.at[pl.ds(0, rows)], recv, tp_send.at[1], tp_recv.at[1], twin)

    def stream(n):
        cols = ds(n * tn, tn)
        return remote(part.at[upper, cols], tiles.at[:, cols], tp_send.at[2 + n], tp_recv.at[2 + n], twin)

    def bring(at):
        other[at(0), :] = recv0[at(0), :]

    each_block(rows, bring)
    scale = 1.0 + f32(gain[...])

    @pl.loop(0, NUM_REQ)
    def _(req):
        @pl.when(req == 1)
        def _():
            incoming.wait_recv()

        def row_block(at):
            src = at(req * rows)
            h = add_parts(hid_in[src, :], own[src, :], other[src, :])
            hid[src, :] = h
            x[at(0), :] = normed(h, scale)

        each_block(rows, row_block)

        @pl.loop(0, nf)
        def _(i):
            slot = lax.rem(i, nb)
            gload(i, slot).wait()
            gate = dot32(x[...], gbuf[slot])
            uload(i, slot).wait()
            act[:, ds(i * tf, tf)] = bf16(gelu_tanh(gate) * dot32(x[...], ubuf[slot]))

            @pl.when(i + nb < nf)
            def _():
                gload(i + nb, slot).start()
                uload(i + nb, slot).start()

            @pl.when((i + nb >= nf) & (i + nb < nf + nd))
            def _():
                dload(i + nb - nf, i + nb - nf).start()

        @pl.loop(0, nn)
        def _(i):
            slot = lax.rem(i, nd)
            dload(i, slot).wait()
            part[ds(req * rows, rows, BLOCK), ds(i * tn, tn)] = bf16(dot32(act[...], dbuf[slot]))

            @pl.when(i + nd < nn)
            def _():
                dload(i + nd, slot).start()

            @pl.when((i + nd >= nn) & (req == 0))
            def _():
                gload(i + nd - nn, i + nd - nn).start()
                uload(i + nd - nn, i + nd - nn).start()

            @pl.when((req == 1) & (i < streamed))
            def _():
                stream(i).start()

        @pl.when(req == 0)
        def _():
            swap.start()

    swap.wait_recv()
    if last:
        def finish(req, others, at_other, cols):
            def image_block(at):
                src = at(req * rows)
                image[req, at(0), cols] = add_parts(hid[src, cols], part[src, cols], others[at(0), at_other])

            def prompt_block(at):
                src = at(req * rows + img_loc)
                prompt[req, at(0), cols] = add_parts(hid[src, cols], part[src, cols], others[at(img_loc), at_other])

            each_block(img_loc, image_block)
            each_block(rows - img_loc, prompt_block)

        finish(0, recv, slice(None), slice(None))
        for n in range(nn):
            cols = pl.ds(n * tn, tn)
            stream(n).wait_recv()
            finish(1, tiles, cols, cols)
    else:
        stream(0).wait_recv()
    incoming.wait_send()
    swap.wait_send()
    for n in range(streamed):
        stream(n).wait_send()


def mlp(hid, own, recv, gain, wg, wu, wd, layer, img_loc, tf=1024, tn=512, nb=2, nd=2):
    rows, width = recv.shape
    ff = wg.shape[2]
    last = layer == NUM_LAYERS - 1
    if last:
        outs = (out(NUM_REQ, img_loc, width), out(NUM_REQ, rows - img_loc, width))
        extra = [vmem(NUM_REQ * rows, width), vmem(NUM_REQ * rows, width), vmem(rows, width), vmem(rows, width)]
    else:
        outs = (out(NUM_REQ * rows, width), out(NUM_REQ * rows, width), out(rows, width), out(rows, tn))
        extra = []
    return pl.pallas_call(
        functools.partial(mlp_kernel, layer, img_loc, tf, tn),
        out_shape=outs,
        in_specs=[VMEM_SPEC] * 4 + [ANY_SPEC] * 3,
        out_specs=(VMEM_SPEC,) * len(outs),
        scratch_shapes=extra + [
            vmem(NUM_REQ * rows, width), vmem(rows, width), vmem(rows, ff),
            vmem(nb, width, tf), vmem(nb, width, tf), vmem(nd, ff, tn),
            DMA((nb,)), DMA((nb,)), DMA((nd,)), DMA((2 + width // tn,)), DMA((2 + width // tn,)),
        ],
        compiler_params=pltpu.CompilerParams(collective_id=NUM_LAYERS + layer, has_side_effects=True, vmem_limit_bytes=63 << 20),
        name=f"mlp{layer}",
    )(hid, own, recv, gain, wg, wu, wd)


def solution(mesh):
    sp_size = mesh.shape["sp"]
    in_specs = (P("dp", "sp", None), P("dp", "sp"), P("dp"), P(), P(), P("tp", None), P(), P(None, None, "tp"), P(), P(), P(None, "tp", None), P(), P(None, None, "tp"), P(None, None, "tp"), P(None, "tp", None))
    out_specs = (P("dp", "sp", None), P("dp", "sp", None), P(None, None, "dp", "sp", None), P(None, None, "dp", "sp", None))

    def device_fn(features, tokens, lengths, proj_w, proj_b, embed, ln_attn, w_query, w_key, w_value, w_out, ln_mlp, w_gate, w_up, w_down):
        img_loc, txt_loc = features.shape[1], tokens.shape[1]
        rows = img_loc + txt_loc
        head_dim = w_key.shape[2]
        shard_idx = lax.axis_index("sp")
        local = jnp.arange(rows)
        positions = jnp.where(local < img_loc, shard_idx * img_loc + local, img_loc * sp_size + shard_idx * txt_loc + local - img_loc)
        inv_freq = np.power(np.float32(ROPE_THETA), -np.arange(head_dim // 2, dtype=np.float32) * np.float32(2.0 / head_dim))
        angles = f32(positions)[:, None] * inv_freq[None, :]
        cos, sin = jnp.cos(angles), jnp.sin(angles)

        sources = start(tokens, features, proj_w, proj_b, embed)
        caches = []
        for layer in range(NUM_LAYERS):
            hid, kv, part, recv = attention(sources, ln_attn[layer:layer + 1], cos, sin, lengths, w_query, w_key, w_value, w_out, layer, img_loc)
            caches.append(kv.reshape(NUM_REQ, rows, 2, head_dim))
            sources = mlp(hid, part, recv, ln_mlp[layer:layer + 1], w_gate, w_up, w_down, layer, img_loc)
        cache = jnp.stack(caches).transpose(0, 3, 1, 2, 4)
        return *sources, cache[:, :, :, :img_loc], cache[:, :, :, img_loc:]

    return jax.shard_map(device_fn, mesh=mesh, in_specs=in_specs, out_specs=out_specs, check_vma=False)
```

```python
import functools
import math
import numpy as np
import jax
import jax.numpy as jnp
from jax import lax
from jax.experimental import pallas as pl
from jax.experimental.pallas import tpu as pltpu
from jax.sharding import PartitionSpec as P

NORM_EPS = 1e-6
ROPE_THETA = 10000.0
NUM_LAYERS = 2
NUM_REQ = 2
BLOCK = 16
GROUP = 8
MASKED = -1e30
MESH_ID = pl.DeviceIdType.MESH
VMEM_SPEC = pl.BlockSpec(memory_space=pltpu.VMEM)
SMEM_SPEC = pl.BlockSpec(memory_space=pltpu.SMEM)
ANY_SPEC = pl.BlockSpec(memory_space=pl.ANY)
HBM_SPEC = pl.BlockSpec(memory_space=pltpu.HBM)
DMA = pltpu.SemaphoreType.DMA


def vmem(*shape):
    return pltpu.VMEM(shape, jnp.bfloat16)


def out(*shape):
    return jax.ShapeDtypeStruct(shape, jnp.bfloat16)


def dot32(a, b):
    return jnp.dot(a, b, preferred_element_type=jnp.float32)


def f32(a):
    return a.astype(jnp.float32)


def bf16(a):
    return a.astype(jnp.bfloat16)


def gelu_tanh(x):
    return x * (0.5 * (1.0 + jnp.tanh(math.sqrt(2.0 / math.pi) * (x + 0.044715 * (x * x * x)))))


def add_parts(hidden, own, other):
    return bf16(f32(hidden) + f32(bf16(f32(own) + f32(other))))


def normed(h, scale):
    h = f32(h)
    return bf16(h * lax.rsqrt(jnp.mean(h * h, axis=-1, keepdims=True) + NORM_EPS) * scale)


def ds(start, size, multiple=None):
    return pl.ds(pl.multiple_of(start, multiple or size), size)


def each_block(rows, body):
    @pl.loop(0, rows // BLOCK)
    def _(blk):
        body(lambda base: ds(base + blk * BLOCK, BLOCK))


def greet(peers):
    barrier = pltpu.get_barrier_semaphore()
    for peer in peers:
        pl.semaphore_signal(barrier, inc=1, device_id=peer, device_id_type=MESH_ID)
    pl.semaphore_wait(barrier, len(peers))


def remote(src, dst, send_sem, recv_sem, peer):
    return pltpu.make_async_remote_copy(src_ref=src, dst_ref=dst, send_sem=send_sem, recv_sem=recv_sem, device_id=peer, device_id_type=MESH_ID)


def start_kernel(ids, id_rows, embed, picked, groups, sem):
    rows_loc = embed.shape[0]
    num = id_rows.shape[1]
    lo = lax.axis_index("tp") * rows_loc
    for req in range(NUM_REQ):
        @pl.loop(0, num, unroll=8)
        def _(i):
            row = jnp.clip(ids[req, i] - lo, 0, rows_loc - 1)
            pltpu.make_async_copy(embed.at[ds(row - (row & (GROUP - 1)), GROUP)], groups.at[req * num + i], sem.at[req]).start()

    line = lax.broadcasted_iota(jnp.int32, (num * GROUP, num), 0)
    lane = lax.broadcasted_iota(jnp.int32, (num * GROUP, num), 1)
    for req in range(NUM_REQ):
        rel = id_rows[req:req + 1, :] - lo
        want = jnp.where((rel >= 0) & (rel < rows_loc), rel & (GROUP - 1), -GROUP * num)
        pick = jnp.where(line - lane * GROUP == want, 1.0, 0.0).astype(jnp.bfloat16)
        mine = groups.at[pl.ds(req * num, num)]
        pltpu.make_async_copy(mine, mine, sem.at[req]).wait()
        rows = mine[...].reshape(num * GROUP, groups.shape[2])
        picked[req * num:(req + 1) * num, :] = bf16(lax.dot_general(pick, rows, (((0,), (0,)), ((), ())), preferred_element_type=jnp.float32))


def start(tokens, embed):
    num, width = tokens.size, embed.shape[1]
    return pl.pallas_call(
        start_kernel,
        out_shape=out(num, width),
        in_specs=[SMEM_SPEC, VMEM_SPEC, ANY_SPEC],
        out_specs=VMEM_SPEC,
        scratch_shapes=[vmem(num, GROUP, width), DMA((NUM_REQ,))],
        compiler_params=pltpu.CompilerParams(vmem_limit_bytes=32 << 20),
        name="start",
    )(tokens, tokens, embed)


def attention_kernel(layer, img_loc, *refs):
    first = layer == 0
    if first:
        picked, features, proj, bias, *refs = refs
    else:
        hid_in, mlp_part, mlp_recv, mlp_tile, kv_before, *refs = refs
    gain, freq, lengths, wq, wk, wv, wo, hid_out, part_out, recv, *refs = refs
    if first:
        kv, *refs = refs
    else:
        cache_image, cache_prompt, *refs = refs
    hid, part, x, arrive, kvs, q, o, cos, sin, wq_buf, wk_buf, wv_buf, wo_buf, lsem, osem, tp_send, tp_recv, sp_send, sp_recv, *refs = refs
    rows = hid.shape[0] // NUM_REQ
    txt_loc = rows - img_loc
    head_dim = wk.shape[2]
    half = head_dim // 2
    heads = wq.shape[2] // head_dim
    width = hid.shape[1]
    me = lax.axis_index("sp")
    twin = {"tp": 1 - lax.axis_index("tp")}
    near, far, cross = [lax.bitwise_xor(me, k) for k in (1, 2, 3)]
    pieces = ((0, img_loc), (img_loc, txt_loc)) if first else ((0, rows),)

    def load(i, src, dst):
        return pltpu.make_async_copy(src, dst, lsem.at[i])

    weights = [load(i, src.at[layer], dst) for i, (src, dst) in enumerate(((wk, wk_buf), (wv, wv_buf), (wq, wq_buf), (wo, wo_buf)))]
    if first:
        feat_buf, proj_buf = refs
        inputs = [load(4 + req, features.at[req], feat_buf.at[req]) for req in range(NUM_REQ)] + [load(6, proj, proj_buf)]
    else:
        own, other = refs
        done = mlp_tile.shape[1]
        lower, upper = pl.ds(0, rows), pl.ds(rows, rows)
        inputs = [load(4, hid_in.at[lower], hid.at[lower]), load(5, mlp_part.at[lower], own.at[lower]), load(6, mlp_recv, other), load(7, hid_in.at[upper], hid.at[upper]), load(8, mlp_part.at[upper], own.at[upper]), load(9, mlp_tile, arrive.at[:, pl.ds(0, done)])]
    for copy in (*inputs[:3], *weights, *inputs[3:]):
        copy.start()
    greet(({"sp": near}, {"sp": far}, twin))
    if first:
        span = [pl.ds(req * txt_loc, txt_loc) for req in range(NUM_REQ)]
        arrivals = [remote(picked.at[span[req]], arrive.at[span[req]], tp_send.at[req], tp_recv.at[req], twin) for req in range(NUM_REQ)]
    else:
        rest = pl.ds(done, width - done)
        arrivals = [remote(mlp_part.at[upper, rest], arrive.at[:, rest], tp_send.at[1], tp_recv.at[1], twin)]
    for arrival in arrivals:
        arrival.start()
    scale = 1.0 + f32(gain[layer:layer + 1, :])

    local = lax.broadcasted_iota(jnp.int32, (rows, half), 0)
    position = jnp.where(local < img_loc, me * img_loc + local, img_loc * 4 + me * txt_loc + local - img_loc)
    angles = f32(position) * freq[...]
    cos[...] = jnp.cos(angles)
    sin[...] = jnp.sin(angles)

    def rope(v, at):
        a, b = v[:, :half], v[:, half:]
        return a * cos[at, :] - b * sin[at, :], b * cos[at, :] + a * sin[at, :]

    def slot(req, k, lo, size):
        return pl.ds((req * 4 + k) * rows + lo, size)

    def sends(req, p):
        lo, size = pieces[p]
        base = (req * len(pieces) + p) * 3
        return [remote(kvs.at[slot(req, src, lo, size)], kvs.at[slot(req, dst, lo, size)], sp_send.at[base + i], sp_recv.at[base + i], {"sp": peer}) for i, (src, dst, peer) in enumerate(((0, 2, far), (0, 1, near), (2, 3, near)))]

    waited = set()

    def once(i):
        if i not in waited:
            waited.add(i)
            weights[i].wait()

    def project(req, p):
        lo, size = pieces[p]
        at = pl.ds(lo, size)
        here = pl.ds(req * rows + lo, size)
        mine = slot(req, 0, lo, size)
        once(0)
        a, b = rope(dot32(x[here, :], wk_buf[...]), at)
        kvs[mine, :half] = bf16(a)
        kvs[mine, half:head_dim] = bf16(b)
        once(1)
        kvs[mine, head_dim:] = bf16(dot32(x[here, :], wv_buf[...]))
        to_far, to_near, _ = sends(req, p)
        to_far.start()
        to_near.start()
        if first:
            kv[here, :] = kvs[mine, :]
        else:
            for j in range(2):
                lanes = pl.ds(j * head_dim, head_dim)
                for src, base in ((kv_before, req * rows), (kvs, req * 4 * rows)):
                    dst = 0 if src is kv_before else 1
                    cache_image[dst, j, req] = src[pl.ds(base, img_loc), lanes]
                    cache_prompt[dst, j, req] = src[pl.ds(base + img_loc, txt_loc), lanes]
        once(2)
        for head in range(heads):
            base = head * head_dim
            a, b = rope(dot32(x[here, :], wq_buf[:, base:base + head_dim]), at)
            q[here, base:base + half] = bf16(bf16(a) * head_dim ** -0.5)
            q[here, base + half:base + head_dim] = bf16(bf16(b) * head_dim ** -0.5)

    col = lax.broadcasted_iota(jnp.int32, (1, 4 * rows), 1)
    slot_of = (col >= rows).astype(jnp.int32) + (col >= 2 * rows).astype(jnp.int32) + (col >= 3 * rows).astype(jnp.int32)
    owner = jnp.where(slot_of == 0, me, jnp.where(slot_of == 1, near, jnp.where(slot_of == 2, far, cross)))
    idx = col - slot_of * rows
    text_pos = jnp.where(idx < img_loc, -1, owner * txt_loc + idx - img_loc)

    def attend(req):
        for p in range(len(pieces)):
            to_far, _, relay = sends(req, p)
            to_far.wait_recv()
            relay.start()
        for p in range(len(pieces)):
            _, to_near, relay = sends(req, p)
            to_near.wait_recv()
            relay.wait_recv()
        valid = text_pos < lengths[req]
        every = pl.ds(req * 4 * rows, 4 * rows)
        here = pl.ds(req * rows, rows)
        for head in range(heads):
            lanes = slice(head * head_dim, (head + 1) * head_dim)
            s = lax.dot_general(q[here, lanes], kvs[every, :head_dim], (((1,), (1,)), ((), ())), preferred_element_type=jnp.float32)
            s = jnp.where(valid, s, MASKED)
            e = jnp.exp(s - jnp.max(s, axis=-1, keepdims=True))
            p = bf16(e * (1.0 / jnp.sum(e, axis=-1, keepdims=True)))
            o[:, lanes] = bf16(dot32(p, kvs[every, head_dim:]))
        once(3)
        tile = 2 * head_dim
        for n in range(width // tile):
            cols = slice(n * tile, (n + 1) * tile)
            part[here, cols] = bf16(dot32(o[...], wo_buf[:, cols]))

    def put(i, src, dst, req):
        here = pl.ds(req * rows, rows)
        return pltpu.make_async_copy(src.at[here], dst.at[here], osem.at[i])

    puts = [put(2 * req + i, src, dst, req) for req in range(NUM_REQ) for i, (src, dst) in enumerate(((hid, hid_out), (part, part_out)))]
    swap = remote(part.at[pl.ds(0, rows)], recv, tp_send.at[2], tp_recv.at[2], twin)

    def keep(at, h):
        hid[at, :] = h
        x[at, :] = normed(h, scale)

    if first:
        for copy in inputs:
            copy.wait()
        for req in range(NUM_REQ):
            for n in range(4):
                cols = slice(n * (width // 4), (n + 1) * (width // 4))
                hid[pl.ds(req * rows, img_loc), cols] = bf16(dot32(feat_buf[req], proj_buf[:, cols]) + f32(bias[cols]).reshape(1, width // 4))

            def image(at):
                src = at(req * rows)
                x[src, :] = normed(hid[src, :], scale)

            each_block(img_loc, image)
            project(req, 0)

    for req in range(NUM_REQ):
        if first:
            arrivals[req].wait_recv()

            def prompt(at):
                src = at(req * txt_loc)
                keep(at(req * rows + img_loc), bf16((f32(picked[src, :]) + f32(arrive[src, :])) * math.sqrt(width)))

            each_block(txt_loc, prompt)
            puts[2 * req].start()
            project(req, 1)
        else:
            for copy in inputs[3 * req:3 * req + 3]:
                copy.wait()
            if req == 1:
                arrivals[0].wait_recv()
            incoming = other if req == 0 else arrive

            def row_block(at):
                src = at(req * rows)
                keep(src, add_parts(hid[src, :], own[src, :], incoming[at(0), :]))

            each_block(rows, row_block)
            puts[2 * req].start()
            project(req, 0)
        attend(req)
        puts[2 * req + 1].start()
        if req == 0:
            swap.start()
    for copy in puts:
        copy.wait()
    swap.wait_recv()
    for copy in (*arrivals, swap, *[c for req in range(NUM_REQ) for p in range(len(pieces)) for c in sends(req, p)]):
        copy.wait_send()


def attention(sources, extra, gain, freq, lengths, wq, wk, wv, wo, layer, rows, img_loc):
    width, qw = wq.shape[1:]
    kw = wk.shape[2]
    txt_loc = rows - img_loc
    total = NUM_REQ * rows
    first = layer == 0
    if first:
        specs = [VMEM_SPEC, HBM_SPEC, HBM_SPEC, VMEM_SPEC]
        outs, out_specs = (out(total, 2 * kw),), (VMEM_SPEC,)
        scratch = [vmem(NUM_REQ, img_loc, extra[0].shape[2]), vmem(*extra[1].shape)]
    else:
        specs = [HBM_SPEC] * 4 + [VMEM_SPEC]
        outs, out_specs = tuple(out(NUM_LAYERS, 2, NUM_REQ, n, kw) for n in (img_loc, txt_loc)), (VMEM_SPEC, VMEM_SPEC)
        scratch = [vmem(total, width), vmem(rows, width)]
    copies = NUM_REQ * 3 * (2 if first else 1)
    return pl.pallas_call(
        functools.partial(attention_kernel, layer, img_loc),
        out_shape=(out(total, width), out(total, width), out(rows, width), *outs),
        in_specs=specs + [VMEM_SPEC] * 2 + [SMEM_SPEC] + [ANY_SPEC] * 4,
        out_specs=(HBM_SPEC,) * 3 + out_specs,
        scratch_shapes=[
            vmem(total, width), vmem(total, width), vmem(total, width), vmem(NUM_REQ * txt_loc if first else rows, width),
            vmem(NUM_REQ * 4 * rows, 2 * kw), vmem(total, qw), vmem(rows, qw),
            pltpu.VMEM((rows, kw // 2), jnp.float32), pltpu.VMEM((rows, kw // 2), jnp.float32),
            vmem(width, qw), vmem(width, kw), vmem(width, kw), vmem(qw, width),
            DMA((10,)), DMA((2 * NUM_REQ,)), DMA((3,)), DMA((3,)), DMA((copies,)), DMA((copies,)), *scratch,
        ],
        compiler_params=pltpu.CompilerParams(collective_id=layer, has_side_effects=True, vmem_limit_bytes=56 << 20),
        name=f"attention{layer}",
    )(*sources, *extra, gain, freq, lengths, wq, wk, wv, wo)


def mlp_kernel(layer, img_loc, tf, tn, hid_in, own_in, recv0, gain, wg, wu, wd, *refs):
    last = layer == NUM_LAYERS - 1
    if last:
        image, prompt, recv, tiles, *refs = refs
    else:
        hid_out, part_out, recv, tiles, *refs = refs
    hid, own, part, other, x, act, gbuf, ubuf, dbuf, lsem, osem, gsem, usem, dsem, tp_send, tp_recv = refs
    rows = recv0.shape[0]
    lower, upper = pl.ds(0, rows), pl.ds(rows, rows)
    inputs = [pltpu.make_async_copy(src, dst, lsem.at[i]) for i, (src, dst) in enumerate(((hid_in.at[lower], hid.at[lower]), (own_in.at[lower], own.at[lower]), (recv0, other.at[lower]), (hid_in.at[upper], hid.at[upper]), (own_in.at[upper], own.at[upper])))]
    for copy in inputs:
        copy.start()
    ff, width = wd.shape[1:]
    nf, nn = ff // tf, width // tn
    nb, nd = gbuf.shape[0], dbuf.shape[0]
    streamed = nn if last else 1
    twin = {"tp": 1 - lax.axis_index("tp")}

    def load(src, buf, sem, tile, i, slot):
        return pltpu.make_async_copy(src.at[layer, :, ds(i * tile, tile)], buf.at[slot], sem.at[slot])

    gload = functools.partial(load, wg, gbuf, gsem, tf)
    uload = functools.partial(load, wu, ubuf, usem, tf)
    dload = functools.partial(load, wd, dbuf, dsem, tn)
    for i in range(nb):
        gload(i, i).start()
        uload(i, i).start()
    greet((twin,))
    incoming = remote(own_in.at[upper], other.at[upper], tp_send.at[0], tp_recv.at[0], twin)
    incoming.start()
    swap = remote(part.at[lower], recv, tp_send.at[1], tp_recv.at[1], twin)

    def stream(n):
        cols = ds(n * tn, tn)
        return remote(part.at[upper, cols], tiles.at[:, cols], tp_send.at[2 + n], tp_recv.at[2 + n], twin)

    scale = 1.0 + f32(gain[layer:layer + 1, :])
    for copy in inputs:
        copy.wait()

    def put(i, src, dst, req):
        here = ds(req * rows, rows, BLOCK)
        return pltpu.make_async_copy(src.at[here], dst.at[here], osem.at[2 * req + i])

    @pl.loop(0, NUM_REQ)
    def _(req):
        @pl.when(req == 1)
        def _():
            incoming.wait_recv()

        def row_block(at):
            src = at(req * rows)
            h = add_parts(hid[src, :], own[src, :], other[src, :])
            hid[src, :] = h
            x[at(0), :] = normed(h, scale)

        each_block(rows, row_block)
        if not last:
            put(0, hid, hid_out, req).start()

        @pl.loop(0, nf)
        def _(i):
            slot = lax.rem(i, nb)
            gload(i, slot).wait()
            gate = dot32(x[...], gbuf[slot])
            uload(i, slot).wait()
            act[:, ds(i * tf, tf)] = bf16(gelu_tanh(gate) * dot32(x[...], ubuf[slot]))

            @pl.when(i + nb < nf)
            def _():
                gload(i + nb, slot).start()
                uload(i + nb, slot).start()

            @pl.when((i + nb >= nf) & (i + nb < nf + nd))
            def _():
                dload(i + nb - nf, i + nb - nf).start()

        @pl.loop(0, nn)
        def _(i):
            slot = lax.rem(i, nd)
            dload(i, slot).wait()
            part[ds(req * rows, rows, BLOCK), ds(i * tn, tn)] = bf16(dot32(act[...], dbuf[slot]))

            @pl.when(i + nd < nn)
            def _():
                dload(i + nd, slot).start()

            @pl.when((i + nd >= nn) & (req == 0))
            def _():
                gload(i + nd - nn, i + nd - nn).start()
                uload(i + nd - nn, i + nd - nn).start()

            @pl.when((req == 1) & (i < streamed))
            def _():
                stream(i).start()

        if not last:
            put(1, part, part_out, req).start()

        @pl.when(req == 0)
        def _():
            swap.start()

    swap.wait_recv()
    if last:
        def finish(req, others, at_other, cols):
            def image_block(at):
                src = at(req * rows)
                image[req, at(0), cols] = add_parts(hid[src, cols], part[src, cols], others[at(0), at_other])

            def prompt_block(at):
                src = at(req * rows + img_loc)
                prompt[req, at(0), cols] = add_parts(hid[src, cols], part[src, cols], others[at(img_loc), at_other])

            each_block(img_loc, image_block)
            each_block(rows - img_loc, prompt_block)

        finish(0, recv, slice(None), slice(None))
        for n in range(nn):
            cols = pl.ds(n * tn, tn)
            stream(n).wait_recv()
            finish(1, tiles, cols, cols)
    else:
        stream(0).wait_recv()
        for req in range(NUM_REQ):
            put(0, hid, hid_out, req).wait()
            put(1, part, part_out, req).wait()
    incoming.wait_send()
    swap.wait_send()
    for n in range(streamed):
        stream(n).wait_send()


def mlp(hid, own, recv, gain, wg, wu, wd, layer, img_loc, tf=1024, tn=512, nb=2, nd=2):
    rows, width = recv.shape
    ff = wg.shape[2]
    last = layer == NUM_LAYERS - 1
    if last:
        outs = (out(NUM_REQ, img_loc, width), out(NUM_REQ, rows - img_loc, width))
        out_specs = (VMEM_SPEC,) * 2
        extra = [vmem(rows, width), vmem(rows, width)]
    else:
        outs = (out(NUM_REQ * rows, width), out(NUM_REQ * rows, width), out(rows, width), out(rows, tn))
        out_specs = (HBM_SPEC,) * 4
        extra = []
    return pl.pallas_call(
        functools.partial(mlp_kernel, layer, img_loc, tf, tn),
        out_shape=outs,
        in_specs=[HBM_SPEC] * 3 + [VMEM_SPEC] + [ANY_SPEC] * 3,
        out_specs=out_specs,
        scratch_shapes=extra + [
            *[vmem(NUM_REQ * rows, width)] * 4, vmem(rows, width), vmem(rows, ff),
            vmem(nb, width, tf), vmem(nb, width, tf), vmem(nd, ff, tn),
            DMA((5,)), DMA((2 * NUM_REQ,)), DMA((nb,)), DMA((nb,)), DMA((nd,)), DMA((2 + width // tn,)), DMA((2 + width // tn,)),
        ],
        compiler_params=pltpu.CompilerParams(collective_id=NUM_LAYERS + layer, has_side_effects=True, vmem_limit_bytes=63 << 20),
        name=f"mlp{layer}",
    )(hid, own, recv, gain, wg, wu, wd)


def solution(mesh):
    in_specs = (P("dp", "sp", None), P("dp", "sp"), P("dp"), P(), P(), P("tp", None), P(), P(None, None, "tp"), P(), P(), P(None, "tp", None), P(), P(None, None, "tp"), P(None, None, "tp"), P(None, "tp", None))
    out_specs = (P("dp", "sp", None), P("dp", "sp", None), P(None, None, "dp", "sp", None), P(None, None, "dp", "sp", None))

    def device_fn(features, tokens, lengths, proj_w, proj_b, embed, ln_attn, w_query, w_key, w_value, w_out, ln_mlp, w_gate, w_up, w_down):
        img_loc = features.shape[1]
        rows = img_loc + tokens.shape[1]
        half = w_key.shape[2] // 2
        freq = np.power(np.float32(ROPE_THETA), -np.arange(half, dtype=np.float32) * np.float32(1.0 / half)).reshape(1, half)
        sources = (start(tokens, embed),)
        extra = (features, proj_w, proj_b)
        for layer in range(NUM_LAYERS):
            hid, part, recv, *caches = attention(sources, extra, ln_attn, freq, lengths, w_query, w_key, w_value, w_out, layer, rows, img_loc)
            extra = tuple(caches)
            sources = mlp(hid, part, recv, ln_mlp, w_gate, w_up, w_down, layer, img_loc)
        return *sources, *caches

    return jax.shard_map(device_fn, mesh=mesh, in_specs=in_specs, out_specs=out_specs, check_vma=False)
```

```python
import functools
import math
import numpy as np
import jax
import jax.numpy as jnp
from jax import lax
from jax.experimental import pallas as pl
from jax.experimental.pallas import tpu as pltpu
from jax.sharding import PartitionSpec as P

NORM_EPS = 1e-6
ROPE_THETA = 10000.0
NUM_LAYERS = 2
NUM_REQ = 2
BLOCK = 16
GROUP = 8
MASKED = -1e30
MESH_ID = pl.DeviceIdType.MESH
VMEM_SPEC = pl.BlockSpec(memory_space=pltpu.VMEM)
SMEM_SPEC = pl.BlockSpec(memory_space=pltpu.SMEM)
ANY_SPEC = pl.BlockSpec(memory_space=pl.ANY)
HBM_SPEC = pl.BlockSpec(memory_space=pltpu.HBM)
DMA = pltpu.SemaphoreType.DMA


def vmem(*shape):
    return pltpu.VMEM(shape, jnp.bfloat16)


def out(*shape):
    return jax.ShapeDtypeStruct(shape, jnp.bfloat16)


def dot32(a, b):
    return jnp.dot(a, b, preferred_element_type=jnp.float32)


def f32(a):
    return a.astype(jnp.float32)


def bf16(a):
    return a.astype(jnp.bfloat16)


def gelu_tanh(x):
    return x * (0.5 * (1.0 + jnp.tanh(math.sqrt(2.0 / math.pi) * (x + 0.044715 * (x * x * x)))))


def add_parts(hidden, own, other):
    return bf16(f32(hidden) + f32(bf16(f32(own) + f32(other))))


def normed(h, scale):
    h = f32(h)
    return bf16(h * lax.rsqrt(jnp.mean(h * h, axis=-1, keepdims=True) + NORM_EPS) * scale)


def ds(start, size, multiple=None):
    return pl.ds(pl.multiple_of(start, multiple or size), size)


def each_block(rows, body):
    @pl.loop(0, rows // BLOCK)
    def _(blk):
        body(lambda base: ds(base + blk * BLOCK, BLOCK))


def greet(peers):
    barrier = pltpu.get_barrier_semaphore()
    for peer in peers:
        pl.semaphore_signal(barrier, inc=1, device_id=peer, device_id_type=MESH_ID)
    pl.semaphore_wait(barrier, len(peers))


def remote(src, dst, send_sem, recv_sem, peer):
    return pltpu.make_async_remote_copy(src_ref=src, dst_ref=dst, send_sem=send_sem, recv_sem=recv_sem, device_id=peer, device_id_type=MESH_ID)


def start_kernel(ids, id_rows, embed, picked, groups, sem):
    rows_loc = embed.shape[0]
    num = id_rows.shape[1]
    lo = lax.axis_index("tp") * rows_loc
    for req in range(NUM_REQ):
        @pl.loop(0, num, unroll=8)
        def _(i):
            row = jnp.clip(ids[req, i] - lo, 0, rows_loc - 1)
            pltpu.make_async_copy(embed.at[ds(row - (row & (GROUP - 1)), GROUP)], groups.at[req * num + i], sem.at[req]).start()

    line = lax.broadcasted_iota(jnp.int32, (num * GROUP, num), 0)
    lane = lax.broadcasted_iota(jnp.int32, (num * GROUP, num), 1)
    for req in range(NUM_REQ):
        rel = id_rows[req:req + 1, :] - lo
        want = jnp.where((rel >= 0) & (rel < rows_loc), rel & (GROUP - 1), -GROUP * num)
        pick = jnp.where(line - lane * GROUP == want, 1.0, 0.0).astype(jnp.bfloat16)
        mine = groups.at[pl.ds(req * num, num)]
        pltpu.make_async_copy(mine, mine, sem.at[req]).wait()
        rows = mine[...].reshape(num * GROUP, groups.shape[2])
        picked[req * num:(req + 1) * num, :] = bf16(lax.dot_general(pick, rows, (((0,), (0,)), ((), ())), preferred_element_type=jnp.float32))


def start(tokens, embed):
    num, width = tokens.size, embed.shape[1]
    return pl.pallas_call(
        start_kernel,
        out_shape=out(num, width),
        in_specs=[SMEM_SPEC, VMEM_SPEC, ANY_SPEC],
        out_specs=VMEM_SPEC,
        scratch_shapes=[vmem(num, GROUP, width), DMA((NUM_REQ,))],
        compiler_params=pltpu.CompilerParams(vmem_limit_bytes=32 << 20),
        name="start",
    )(tokens, tokens, embed)


def attention_kernel(layer, img_loc, *refs):
    first = layer == 0
    if first:
        picked, features, proj, bias, *refs = refs
    else:
        hid_in, mlp_part, mlp_recv, mlp_tile, wo_twin, kv_before, *refs = refs
    gain, freq, lengths, wq, wk, wv, wo, hid_out, part_out, *refs = refs
    if first:
        recv, kv, *refs = refs
    else:
        cache_image, cache_prompt, *refs = refs
    hid, part, x, arrive, kvs, q, o, cos, sin, wq_buf, wk_buf, wv_buf, wo_buf, lsem, osem, tp_send, tp_recv, sp_send, sp_recv, *refs = refs
    rows = hid.shape[0] // NUM_REQ
    txt_loc = rows - img_loc
    head_dim = wk.shape[2]
    half = head_dim // 2
    heads = wq.shape[2] // head_dim
    width = hid.shape[1]
    me = lax.axis_index("sp")
    twin = {"tp": 1 - lax.axis_index("tp")}
    near, far, cross = [lax.bitwise_xor(me, k) for k in (1, 2, 3)]
    pieces = ((0, img_loc), (img_loc, txt_loc)) if first else ((0, rows),)

    def load(i, src, dst):
        return pltpu.make_async_copy(src, dst, lsem.at[i])

    weights = [load(i, src.at[layer], dst) for i, (src, dst) in enumerate(((wk, wk_buf), (wv, wv_buf), (wq, wq_buf), (wo, wo_buf)))]
    if first:
        feat_buf, proj_buf = refs
        inputs = [load(4 + req, features.at[req], feat_buf.at[req]) for req in range(NUM_REQ)] + [load(6, proj, proj_buf)]
    else:
        own, other, o_first, o_twin, wo_twin_buf = refs
        done = mlp_tile.shape[1]
        lower, upper = pl.ds(0, rows), pl.ds(rows, rows)
        inputs = [load(4, hid_in.at[lower], hid.at[lower]), load(5, mlp_part.at[lower], own.at[lower]), load(6, mlp_recv, other), load(7, hid_in.at[upper], hid.at[upper]), load(8, mlp_part.at[upper], own.at[upper]), load(9, mlp_tile, arrive.at[:, pl.ds(0, done)])]
        share = wo_twin_buf.shape[0] // 4
        quarters = [ds(k * share, share) for k in (me, near, far)]
        inputs += [load(10 + k, wo_twin.at[at], wo_twin_buf.at[at]) for k, at in enumerate(quarters)]
        last_quarter = remote(wo_twin.at[quarters[2]], wo_twin_buf.at[quarters[2]], sp_send.at[3 * NUM_REQ], sp_recv.at[3 * NUM_REQ], {"sp": near})
    for copy in (*inputs[:3], *weights, *inputs[3:]):
        copy.start()
    greet(({"sp": near}, {"sp": far}, twin))
    if first:
        span = [pl.ds(req * txt_loc, txt_loc) for req in range(NUM_REQ)]
        arrivals = [remote(picked.at[span[req]], arrive.at[span[req]], tp_send.at[req], tp_recv.at[req], twin) for req in range(NUM_REQ)]
    else:
        rest = pl.ds(done, width - done)
        arrivals = [remote(mlp_part.at[upper, rest], arrive.at[:, rest], tp_send.at[1], tp_recv.at[1], twin)]
    for arrival in arrivals:
        arrival.start()
    if not first:
        last_quarter.start()
    scale = 1.0 + f32(gain[layer:layer + 1, :])

    local = lax.broadcasted_iota(jnp.int32, (rows, half), 0)
    position = jnp.where(local < img_loc, me * img_loc + local, img_loc * 4 + me * txt_loc + local - img_loc)
    angles = f32(position) * freq[...]
    cos[...] = jnp.cos(angles)
    sin[...] = jnp.sin(angles)

    def rope(v, at):
        a, b = v[:, :half], v[:, half:]
        return a * cos[at, :] - b * sin[at, :], b * cos[at, :] + a * sin[at, :]

    def slot(req, k, lo, size):
        return pl.ds((req * 4 + k) * rows + lo, size)

    def sends(req, p):
        lo, size = pieces[p]
        base = (req * len(pieces) + p) * 3
        return [remote(kvs.at[slot(req, src, lo, size)], kvs.at[slot(req, dst, lo, size)], sp_send.at[base + i], sp_recv.at[base + i], {"sp": peer}) for i, (src, dst, peer) in enumerate(((0, 2, far), (0, 1, near), (2, 3, near)))]

    waited = set()

    def once(i):
        if i not in waited:
            waited.add(i)
            weights[i].wait()

    def project(req, p):
        lo, size = pieces[p]
        at = pl.ds(lo, size)
        here = pl.ds(req * rows + lo, size)
        mine = slot(req, 0, lo, size)
        once(0)
        a, b = rope(dot32(x[here, :], wk_buf[...]), at)
        kvs[mine, :half] = bf16(a)
        kvs[mine, half:head_dim] = bf16(b)
        once(1)
        kvs[mine, head_dim:] = bf16(dot32(x[here, :], wv_buf[...]))
        to_far, to_near, _ = sends(req, p)
        to_far.start()
        to_near.start()
        if first:
            kv[here, :] = kvs[mine, :]
        else:
            for j in range(2):
                lanes = pl.ds(j * head_dim, head_dim)
                for src, base in ((kv_before, req * rows), (kvs, req * 4 * rows)):
                    dst = 0 if src is kv_before else 1
                    cache_image[dst, j, req] = src[pl.ds(base, img_loc), lanes]
                    cache_prompt[dst, j, req] = src[pl.ds(base + img_loc, txt_loc), lanes]
        once(2)
        for head in range(heads):
            base = head * head_dim
            a, b = rope(dot32(x[here, :], wq_buf[:, base:base + head_dim]), at)
            q[here, base:base + half] = bf16(bf16(a) * head_dim ** -0.5)
            q[here, base + half:base + head_dim] = bf16(bf16(b) * head_dim ** -0.5)

    col = lax.broadcasted_iota(jnp.int32, (1, 4 * rows), 1)
    slot_of = (col >= rows).astype(jnp.int32) + (col >= 2 * rows).astype(jnp.int32) + (col >= 3 * rows).astype(jnp.int32)
    owner = jnp.where(slot_of == 0, me, jnp.where(slot_of == 1, near, jnp.where(slot_of == 2, far, cross)))
    idx = col - slot_of * rows
    text_pos = jnp.where(idx < img_loc, -1, owner * txt_loc + idx - img_loc)

    def attend(req, o):
        for p in range(len(pieces)):
            to_far, _, relay = sends(req, p)
            to_far.wait_recv()
            relay.start()
        for p in range(len(pieces)):
            _, to_near, relay = sends(req, p)
            to_near.wait_recv()
            relay.wait_recv()
        valid = text_pos < lengths[req]
        every = pl.ds(req * 4 * rows, 4 * rows)
        here = pl.ds(req * rows, rows)
        for head in range(heads):
            lanes = slice(head * head_dim, (head + 1) * head_dim)
            s = lax.dot_general(q[here, lanes], kvs[every, :head_dim], (((1,), (1,)), ((), ())), preferred_element_type=jnp.float32)
            s = jnp.where(valid, s, MASKED)
            e = jnp.exp(s - jnp.max(s, axis=-1, keepdims=True))
            p = bf16(e * (1.0 / jnp.sum(e, axis=-1, keepdims=True)))
            o[:, lanes] = bf16(dot32(p, kvs[every, head_dim:]))
        once(3)

    tile = 2 * head_dim
    out_tiles = [slice(n * tile, (n + 1) * tile) for n in range(width // tile)]

    def project_out(req):
        here = pl.ds(req * rows, rows)
        for cols in out_tiles:
            part[here, cols] = bf16(dot32(o[...], wo_buf[:, cols]))

    def put(i, src, dst, req):
        here = pl.ds(req * rows, rows)
        return pltpu.make_async_copy(src.at[here], dst.at[here], osem.at[i])

    puts = [put(2 * req + i, src, dst, req) for req in range(NUM_REQ) for i, (src, dst) in enumerate(((hid, hid_out), (part, part_out)))]
    swap = remote(part.at[pl.ds(0, rows)], recv, tp_send.at[2], tp_recv.at[2], twin) if first else remote(o_first, o_twin, tp_send.at[2], tp_recv.at[2], twin)

    def keep(at, h):
        hid[at, :] = h
        x[at, :] = normed(h, scale)

    if first:
        for copy in inputs:
            copy.wait()
        for req in range(NUM_REQ):
            for n in range(4):
                cols = slice(n * (width // 4), (n + 1) * (width // 4))
                hid[pl.ds(req * rows, img_loc), cols] = bf16(dot32(feat_buf[req], proj_buf[:, cols]) + f32(bias[cols]).reshape(1, width // 4))

            def image(at):
                src = at(req * rows)
                x[src, :] = normed(hid[src, :], scale)

            each_block(img_loc, image)
            project(req, 0)

    for req in range(NUM_REQ):
        if first:
            arrivals[req].wait_recv()

            def prompt(at):
                src = at(req * txt_loc)
                keep(at(req * rows + img_loc), bf16((f32(picked[src, :]) + f32(arrive[src, :])) * math.sqrt(width)))

            each_block(txt_loc, prompt)
            puts[2 * req].start()
            project(req, 1)
        else:
            for copy in inputs[3 * req:3 * req + 3]:
                copy.wait()
            if req == 1:
                arrivals[0].wait_recv()
            incoming = other if req == 0 else arrive

            def row_block(at):
                src = at(req * rows)
                keep(src, add_parts(hid[src, :], own[src, :], incoming[at(0), :]))

            each_block(rows, row_block)
            if req == 1:
                puts[2].start()
            project(req, 0)
        if first or req == 1:
            attend(req, o)
            project_out(req)
            puts[2 * req + 1].start()
        else:
            attend(req, o_first)
        if req == 0:
            swap.start()
    swap.wait_recv()
    if not first:
        for copy in inputs[6:]:
            copy.wait()
        last_quarter.wait()
        for cols in out_tiles:
            total = dot32(o_first[...], wo_buf[:, cols]) + dot32(o_twin[...], wo_twin_buf[:, cols])
            hid[:rows, cols] = bf16(f32(hid[:rows, cols]) + f32(bf16(total)))
        puts[0].start()
        puts = [puts[0], puts[2], puts[3]]
    for copy in puts:
        copy.wait()
    for copy in (*arrivals, swap, *[c for req in range(NUM_REQ) for p in range(len(pieces)) for c in sends(req, p)]):
        copy.wait_send()


def attention(sources, extra, gain, freq, lengths, wq, wk, wv, wo, layer, rows, img_loc):
    width, qw = wq.shape[1:]
    kw = wk.shape[2]
    txt_loc = rows - img_loc
    total = NUM_REQ * rows
    first = layer == 0
    if first:
        specs = [VMEM_SPEC, HBM_SPEC, HBM_SPEC, VMEM_SPEC]
        outs, out_specs = (out(rows, width), out(total, 2 * kw)), (HBM_SPEC, VMEM_SPEC)
        scratch = [vmem(NUM_REQ, img_loc, extra[0].shape[2]), vmem(*extra[1].shape)]
    else:
        specs = [HBM_SPEC] * 5 + [VMEM_SPEC]
        outs, out_specs = tuple(out(NUM_LAYERS, 2, NUM_REQ, n, kw) for n in (img_loc, txt_loc)), (VMEM_SPEC, VMEM_SPEC)
        scratch = [vmem(total, width), vmem(rows, width), vmem(rows, qw), vmem(rows, qw), vmem(qw, width)]
    copies = NUM_REQ * 3 * 2
    return pl.pallas_call(
        functools.partial(attention_kernel, layer, img_loc),
        out_shape=(out(total, width), out(total, width), *outs),
        in_specs=specs + [VMEM_SPEC] * 2 + [SMEM_SPEC] + [ANY_SPEC] * 4,
        out_specs=(HBM_SPEC,) * 2 + out_specs,
        scratch_shapes=[
            vmem(total, width), vmem(total, width), vmem(total, width), vmem(NUM_REQ * txt_loc if first else rows, width),
            vmem(NUM_REQ * 4 * rows, 2 * kw), vmem(total, qw), vmem(rows, qw),
            pltpu.VMEM((rows, kw // 2), jnp.float32), pltpu.VMEM((rows, kw // 2), jnp.float32),
            vmem(width, qw), vmem(width, kw), vmem(width, kw), vmem(qw, width),
            DMA((13,)), DMA((2 * NUM_REQ,)), DMA((3,)), DMA((3,)), DMA((copies,)), DMA((copies,)), *scratch,
        ],
        compiler_params=pltpu.CompilerParams(collective_id=layer, has_side_effects=True, vmem_limit_bytes=56 << 20),
        name=f"attention{layer}",
    )(*sources, *extra, gain, freq, lengths, wq, wk, wv, wo)


def mlp_kernel(layer, img_loc, tf, tn, hid_in, own_in, *refs):
    last = layer == NUM_LAYERS - 1
    if last:
        gain, wg, wu, wd, image, prompt, recv, tiles, *refs = refs
    else:
        recv0, wo, gain, wg, wu, wd, hid_out, part_out, recv, tiles, wo_twin, *refs = refs
    hid, own, part, other, x, act, gbuf, ubuf, dbuf, lsem, osem, gsem, usem, dsem, tp_send, tp_recv, w_send, w_recv = refs
    rows = hid_in.shape[0] // NUM_REQ
    lower, upper = pl.ds(0, rows), pl.ds(rows, rows)
    inputs = [pltpu.make_async_copy(src, dst, lsem.at[i]) for i, (src, dst) in enumerate(((hid_in.at[lower], hid.at[lower]), (hid_in.at[upper], hid.at[upper]), (own_in.at[upper], own.at[upper]), *(() if last else ((own_in.at[lower], own.at[lower]), (recv0, other.at[lower])))))]
    for copy in inputs:
        copy.start()
    ff, width = wd.shape[1:]
    nf, nn = ff // tf, width // tn
    nb, nd = gbuf.shape[0], dbuf.shape[0]
    pieces = [(n * tn, tn) for n in range(nn)] if last else [(0, tn)]
    twin = {"tp": 1 - lax.axis_index("tp")}
    me = lax.axis_index("sp")
    near, far = lax.bitwise_xor(me, 1), lax.bitwise_xor(me, 2)

    def load(src, buf, sem, tile, i, slot):
        return pltpu.make_async_copy(src.at[layer, :, ds(i * tile, tile)], buf.at[slot], sem.at[slot])

    gload = functools.partial(load, wg, gbuf, gsem, tf)
    uload = functools.partial(load, wu, ubuf, usem, tf)
    dload = functools.partial(load, wd, dbuf, dsem, tn)
    for i in range(nb):
        gload(i, i).start()
        uload(i, i).start()
    greet((twin,) if last else (twin, {"sp": near}, {"sp": far}))
    incoming = remote(own_in.at[upper], other.at[upper], tp_send.at[0], tp_recv.at[0], twin)
    incoming.start()
    swap = remote(part.at[lower], recv, tp_send.at[1], tp_recv.at[1], twin)

    def stream(n):
        cols = pl.ds(*pieces[n])
        return remote(part.at[upper, cols], tiles.at[:, cols], tp_send.at[2 + n], tp_recv.at[2 + n], twin)

    if not last:
        share = wo.shape[1] // 4
        mine = ds(me * share, share)
        ahead = wo.at[layer + 1, mine]
        hops = [remote(src, wo_twin.at[mine], w_send.at[i], w_recv.at[i], peer) for i, (src, peer) in enumerate(((ahead, twin), (wo_twin.at[mine], {"sp": far}), (wo_twin.at[mine], {"sp": near})))]

    scale = 1.0 + f32(gain[layer:layer + 1, :])
    for copy in inputs:
        copy.wait()

    def put(i, src, dst, req):
        here = ds(req * rows, rows, BLOCK)
        return pltpu.make_async_copy(src.at[here], dst.at[here], osem.at[2 * req + i])

    @pl.loop(0, NUM_REQ)
    def _(req):
        @pl.when(req == 1)
        def _():
            incoming.wait_recv()

        def row_block(at):
            src = at(req * rows)
            h = add_parts(hid[src, :], own[src, :], other[src, :])
            hid[src, :] = h
            x[at(0), :] = normed(h, scale)

        def ready_block(at):
            x[at(0), :] = normed(hid[at(0), :], scale)

        if last:
            pl.when(req == 0)(lambda: each_block(rows, ready_block))
            pl.when(req == 1)(lambda: each_block(rows, row_block))
        else:
            each_block(rows, row_block)
            put(0, hid, hid_out, req).start()

        @pl.loop(0, nf)
        def _(i):
            slot = lax.rem(i, nb)
            gload(i, slot).wait()
            if not last:
                pl.when((req == 0) & (i == nf // 2))(hops[0].start)

                @pl.when((req == 1) & (i == nf // 2))
                def _():
                    hops[0].wait_recv()
                    hops[1].start()
                    hops[2].start()

            gate = dot32(x[...], gbuf[slot])

            @pl.when(i + nb < nf)
            def _():
                gload(i + nb, slot).start()

            uload(i, slot).wait()
            act[:, ds(i * tf, tf)] = bf16(gelu_tanh(gate) * dot32(x[...], ubuf[slot]))

            @pl.when(i + nb < nf)
            def _():
                uload(i + nb, slot).start()

            @pl.when((i + nb >= nf) & (i + nb < nf + nd))
            def _():
                dload(i + nb - nf, i + nb - nf).start()

        @pl.loop(0, nn)
        def _(i):
            slot = lax.rem(i, nd)
            dload(i, slot).wait()
            part[ds(req * rows, rows, BLOCK), ds(i * tn, tn)] = bf16(dot32(act[...], dbuf[slot]))

            @pl.when(i + nd < nn)
            def _():
                dload(i + nd, slot).start()

            @pl.when((i + nd >= nn) & (req == 0))
            def _():
                gload(i + nd - nn, i + nd - nn).start()
                uload(i + nd - nn, i + nd - nn).start()

            for n, (col, _) in enumerate(pieces):
                pl.when((req == 1) & (i == col // tn))(stream(n).start)

        if not last:
            put(1, part, part_out, req).start()

        @pl.when(req == 0)
        def _():
            swap.start()

    swap.wait_recv()
    if last:
        def finish(req, others, at_other, cols):
            def image_block(at):
                src = at(req * rows)
                image[req, at(0), cols] = add_parts(hid[src, cols], part[src, cols], others[at(0), at_other])

            def prompt_block(at):
                src = at(req * rows + img_loc)
                prompt[req, at(0), cols] = add_parts(hid[src, cols], part[src, cols], others[at(img_loc), at_other])

            each_block(img_loc, image_block)
            each_block(rows - img_loc, prompt_block)

        finish(0, recv, slice(None), slice(None))
        for n in range(nn):
            cols = pl.ds(n * tn, tn)
            stream(n).wait_recv()
            finish(1, tiles, cols, cols)
    else:
        for n in range(len(pieces)):
            stream(n).wait_recv()
        hops[1].wait_recv()
        hops[2].wait_recv()
        for hop in hops:
            hop.wait_send()
        for req in range(NUM_REQ):
            put(0, hid, hid_out, req).wait()
            put(1, part, part_out, req).wait()
    incoming.wait_send()
    swap.wait_send()
    for n in range(len(pieces)):
        stream(n).wait_send()


def mlp(sources, gain, wg, wu, wd, layer, img_loc, tf=1024, tn=512, nb=2, nd=2):
    rows, width = sources[0].shape[0] // NUM_REQ, sources[0].shape[1]
    ff = wg.shape[2]
    last = layer == NUM_LAYERS - 1
    if last:
        outs = (out(NUM_REQ, img_loc, width), out(NUM_REQ, rows - img_loc, width))
        out_specs = (VMEM_SPEC,) * 2
        extra = [vmem(rows, width), vmem(rows, width)]
    else:
        outs = (out(NUM_REQ * rows, width), out(NUM_REQ * rows, width), out(rows, width), out(rows, tn), out(*sources[3].shape[1:]))
        out_specs = (HBM_SPEC,) * 5
        extra = []
    return pl.pallas_call(
        functools.partial(mlp_kernel, layer, img_loc, tf, tn),
        out_shape=outs,
        in_specs=[HBM_SPEC] * len(sources) + [VMEM_SPEC] + [ANY_SPEC] * 3,
        out_specs=out_specs,
        scratch_shapes=extra + [
            *[vmem(NUM_REQ * rows, width)] * 4, vmem(rows, width), vmem(rows, ff),
            vmem(nb, width, tf), vmem(nb, width, tf), vmem(nd, ff, tn),
            DMA((5,)), DMA((2 * NUM_REQ,)), DMA((nb,)), DMA((nb,)), DMA((nd,)), DMA((2 + width // tn,)), DMA((2 + width // tn,)), DMA((3,)), DMA((3,)),
        ],
        compiler_params=pltpu.CompilerParams(collective_id=NUM_LAYERS + layer, has_side_effects=True, vmem_limit_bytes=63 << 20),
        name=f"mlp{layer}",
    )(*sources, gain, wg, wu, wd)


def solution(mesh):
    in_specs = (P("dp", "sp", None), P("dp", "sp"), P("dp"), P(), P(), P("tp", None), P(), P(None, None, "tp"), P(), P(), P(None, "tp", None), P(), P(None, None, "tp"), P(None, None, "tp"), P(None, "tp", None))
    out_specs = (P("dp", "sp", None), P("dp", "sp", None), P(None, None, "dp", "sp", None), P(None, None, "dp", "sp", None))

    def device_fn(features, tokens, lengths, proj_w, proj_b, embed, ln_attn, w_query, w_key, w_value, w_out, ln_mlp, w_gate, w_up, w_down):
        img_loc = features.shape[1]
        rows = img_loc + tokens.shape[1]
        half = w_key.shape[2] // 2
        freq = np.power(np.float32(ROPE_THETA), -np.arange(half, dtype=np.float32) * np.float32(1.0 / half)).reshape(1, half)
        sources = (start(tokens, embed),)
        extra = (features, proj_w, proj_b)
        for layer in range(NUM_LAYERS):
            hid, part, *caches = attention(sources, extra, ln_attn, freq, lengths, w_query, w_key, w_value, w_out, layer, rows, img_loc)
            sources = (hid, part)
            if layer == 0:
                recv, *extra = caches
                sources = (hid, part, recv, w_out)
            sources = mlp(sources, ln_mlp, w_gate, w_up, w_down, layer, img_loc)
        return *sources, *caches

    return jax.shard_map(device_fn, mesh=mesh, in_specs=in_specs, out_specs=out_specs, check_vma=False)
```
